32 devices in a mesh: replica: 2 (over y), expert: 8 (over z, core), tensor: 2 (over x).
Axes of the slice: x: 2, y: 2, z: 4, core: 2. Of those that a mesh axis runs over, the one named last changes fastest.
Arguments:
- delta: bfloat16 [2, 128, 4, 14336], P('replica', 'expert', None, 'tensor'), may hold values from -6 to 6
- step_offsets: int32 [2], replicated, may hold values from 0 to 15, as said below
- block_map: int32 [128], replicated, may hold values from 0 to 127, as said below
- master_params: float32 [128, 4, 14336], P('expert', 'replica', 'tensor'), may hold values from -6 to 6
- first_moment: float32 [128, 4, 14336], P('expert', 'replica', 'tensor'), may hold values from -2 to 2
- second_moment: float32 [128, 4, 14336], P('expert', 'replica', 'tensor'), may hold values from 0.01 to 1
Outputs:
- new_params: bfloat16 [128, 4, 14336], P('expert', 'replica')
- new_first: float32 [128, 4, 14336], P('expert', 'replica', 'tensor')
- new_second: float32 [128, 4, 14336], P('expert', 'replica', 'tensor')
The draws below stay inside these ranges and needn't reach their ends.
Inputs may be any that keep to these rules, and one draw needn't show every extreme that they name: `block_map`: A permutation of the block indices onto owner slots; slot s belongs to expert index s // 16, and the blocks b with b // 16 = i go in equal numbers to every expert index. `step_offsets`: the replica groups' offsets are distinct.
All inputs are finite; a program needn't handle non-finite values.
Results may differ from the reference program's by a relative error of at most 0.0035.
Values may be sent and summed in bfloat16 or wider, within the bound.
A program may use at most 64 MiB of HBM per device.

```python
import math
import jax
import jax.numpy as jnp
from jax import lax

FF = 14336
BLK_DEV = 16
BR = 4
BLOCKS = 128
REPLICAS = 2


def shuffled(key_one):
    return jax.random.permutation(key_one, BLK_DEV)


def draw_block_map(key, part):
    owners = BLOCKS // BLK_DEV
    first_key = jax.random.fold_in(key, 11)
    second_key = jax.random.fold_in(key, 23)
    source_perm = jax.vmap(shuffled)(jax.random.split(first_key, owners)).astype(jnp.int32)
    target = source_perm % owners
    ordinal = source_perm // owners
    sources = jnp.arange(owners, dtype=jnp.int32)[:, None]
    arrival = sources * (BLK_DEV // owners) + ordinal
    owner_perm = jax.vmap(shuffled)(jax.random.split(second_key, owners)).astype(jnp.int32)
    slot_ids = owner_perm[target, arrival]
    return (target * BLK_DEV + slot_ids).reshape(BLOCKS).astype(jnp.int32)


def draw_step_offsets(key, part):
    inner_key = jax.random.fold_in(key, 37)
    order_key = jax.random.fold_in(key, 41)
    middle = jax.random.permutation(inner_key, jnp.arange(1, 15, dtype=jnp.int32))[:REPLICAS - 2]
    ends = jnp.array([0, 15], dtype=jnp.int32)
    values = jnp.concatenate([ends, middle.astype(jnp.int32)])
    return jax.random.permutation(order_key, values).astype(jnp.int32)


def spiked(drawn, stream_key, source, target, blocks, factor):
    owner, partner = [(jnp.arange(drawn.shape[position]) // (drawn.shape[position] // blocks)).reshape([-1 if axis == position else 1 for axis in range(drawn.ndim)]) for position in (source, target)]
    chosen = jax.random.permutation(stream_key, blocks)[partner]
    strong = (owner == chosen) | (owner == (partner + blocks // 2) % blocks)
    return jnp.where(strong, factor * drawn, drawn)


def shard_levels(own_key, shape, shards, low, high):
    factor_of = 1.0
    for axis_at, parts in shards:
        heights = jax.random.uniform(jax.random.fold_in(jax.random.fold_in(own_key, 6), axis_at), (parts,), jnp.float32, low / len(shards), high / len(shards))
        factor_of = factor_of * jnp.repeat(jnp.exp(heights), shape[axis_at] // parts).reshape((-1,) + (1,) * (len(shape) - 1 - axis_at))
    return factor_of


def noise(own_key, dims, scale, most, pieces=(), held_as=jnp.bfloat16):
    level = shard_levels(own_key, dims, pieces, -0.22, 0.18) if pieces else 1.0
    drawn = jax.random.normal(own_key, dims, jnp.float32) * scale * level
    return jnp.minimum(jnp.maximum(drawn, -most), most).astype(held_as)


def bell_draw_with(own_key, extent, width, limit, shards, heavy, held_as=jnp.bfloat16):
    values = width * jax.random.normal(own_key, extent, jnp.float32)
    if shards:
        values = values * shard_levels(own_key, extent, shards, -0.22, 0.18)
    return jnp.clip(spiked(values, jax.random.fold_in(own_key, 3), *heavy), -limit, limit).astype(held_as)


def setup_inputs(seed: int = 0) -> dict:
    key_list = jax.random.split(jax.random.key(seed), 7)
    return {
        "delta": bell_draw_with(key_list[0], (REPLICAS, BLOCKS, BR, FF), 1.0, 6.0, ((0, 2), (1, 8), (3, 2)), (0, 2, 2, 2.0)),
        "step_offsets": draw_step_offsets(jax.random.fold_in(key_list[6], 71), 0),
        "block_map": draw_block_map(jax.random.fold_in(key_list[6], 71), 0),
        "master_params": noise(key_list[3], (BLOCKS, BR, FF), 1.0, 6.0, ((0, 8), (1, 2), (2, 2)), jnp.float32),
        "first_moment": noise(key_list[4], (BLOCKS, BR, FF), 0.3, 2.0, ((0, 8), (1, 2), (2, 2)), jnp.float32),
        "second_moment": jnp.clip(jnp.exp(math.log(1.0) - 4.6051702 * jax.random.uniform(key_list[5], (BLOCKS, BR, FF), jnp.float32) ** shard_levels(key_list[5], (BLOCKS, BR, FF), ((0, 8), (1, 2), (2, 2)), -0.2, 0.2)), 0.01, 1.0),
    }


beta_one = 0.9
beta_two = 0.99
outer_rate = 0.7
outer_round = 20
epsilon = 1e-08

def replica_weights(step_offsets):
    reciprocal = 1.0 / (1.0 + step_offsets.astype(jnp.float32))
    return reciprocal / jnp.sum(reciprocal)

def adam_update(gradient, master_params, first_moment, second_moment):
    new_first = beta_one * first_moment + (1.0 - beta_one) * gradient
    new_second = beta_two * second_moment + (1.0 - beta_two) * gradient * gradient
    fix_one = 1.0 - beta_one ** outer_round
    fix_two = 1.0 - beta_two ** outer_round
    update_step = new_first / fix_one / (jnp.sqrt(new_second / fix_two) + epsilon)
    new_params = (master_params - outer_rate * update_step).astype(jnp.bfloat16)
    return (new_params, new_first, new_second)

def reference(delta, step_offsets, block_map, master_params, first_moment, second_moment):
    weights = replica_weights(step_offsets)

    def add_replica(replica_id, running):
        slice_rows = lax.dynamic_index_in_dim(delta, replica_id, 0, keepdims=False).astype(jnp.float32)
        scaled = (slice_rows * weights[replica_id]).astype(jnp.bfloat16)
        scaled = lax.optimization_barrier(scaled)
        return running + scaled.astype(jnp.float32)
    pseudo = lax.fori_loop(0, REPLICAS, add_replica, jnp.zeros(delta.shape[1:], jnp.float32))
    inverse = jnp.argsort(block_map).astype(jnp.int32)
    gradient = pseudo[inverse]
    new_params, new_first, new_second = adam_update(gradient, master_params, first_moment, second_moment)
    return (new_params, new_first, new_second)
```

```python
import functools

import jax
import jax.numpy as jnp
from jax import lax
from jax.experimental import pallas as pl
from jax.experimental.pallas import tpu as pltpu
from jax.sharding import PartitionSpec as P

beta_one = 0.9
beta_two = 0.99
outer_rate = 0.7
outer_round = 20
epsilon = 1e-08

LANES = 128
CHUNK = 8
EDGE = 4
LAG = 2
UNROLL = 16
MESH = pl.DeviceIdType.MESH


def flipped(mine, d, size):
    if size & (size - 1):
        return lax.rem(mine + d, size)
    peer = mine
    bit = 1
    while bit < size:
        if d & bit:
            peer = peer + bit * (1 - 2 * lax.rem(lax.div(mine, bit), 2))
        bit *= 2
    return peer


def kernel(
    sizes,
    block_map_far,
    step_offsets_far,
    delta,
    master_params,
    first_moment,
    second_moment,
    params,
    new_first,
    new_second,
    master,
    first,
    second,
    block_map,
    step_offsets,
    order,
    slots,
    places,
    index_sem,
    load_sem,
    state_sem,
    y_send,
    y_recv,
    z_send,
    z_recv,
    x_send,
    x_recv,
    *buffers,
):
    replicas, experts, tensors, chunks, blocks, pairs, rows = sizes
    count = len(chunks)
    stage = buffers[:count]
    arrived = buffers[count : 2 * count]
    outgoing = buffers[2 * count : 3 * count]
    incoming = buffers[3 * count :]
    my_replica = lax.axis_index("replica")
    my_expert = lax.axis_index("expert")
    my_tensor = lax.axis_index("tensor")
    columns = sum(chunks)
    starts = [sum(chunks[:c]) for c in range(count)]

    def load(c, d):
        replica = lax.rem(my_replica + d, replicas)
        return pltpu.make_async_copy(
            delta.at[:, pl.ds(starts[c], chunks[c]), replica],
            stage[c].at[d],
            load_sem.at[c, d],
        )

    def y_copy(c, d):
        return pltpu.make_async_remote_copy(
            src_ref=stage[c].at[d],
            dst_ref=arrived[c].at[d - 1],
            send_sem=y_send,
            recv_sem=y_recv.at[c],
            device_id={"replica": lax.rem(my_replica + d, replicas)},
            device_id_type=MESH,
        )

    def z_copy(c, d):
        peer = flipped(my_expert, d, experts)
        return pltpu.make_async_remote_copy(
            src_ref=outgoing[c].at[pl.ds(peer * pairs, pairs)],
            dst_ref=incoming[c].at[pl.ds(my_expert * pairs, pairs)],
            send_sem=z_send,
            recv_sem=z_recv.at[c],
            device_id={"expert": peer},
            device_id_type=MESH,
        )

    def x_copy(c, d):
        part = params.at[:, pl.ds(my_tensor * columns + starts[c], chunks[c])]
        return pltpu.make_async_remote_copy(
            src_ref=part,
            dst_ref=part,
            send_sem=x_send,
            recv_sem=x_recv,
            device_id={"tensor": lax.rem(my_tensor + d, tensors)},
            device_id_type=MESH,
        )

    def all_of(ref, sem):
        return pltpu.make_async_copy(ref, ref, sem)

    barrier = pltpu.get_barrier_semaphore()
    axes = (("expert", my_expert, experts), ("replica", my_replica, replicas), ("tensor", my_tensor, tensors))
    for axis, mine, size in axes:
        for d in reversed(range(1, size)):
            pl.semaphore_signal(
                barrier, inc=1, device_id={axis: lax.rem(mine + d, size)}, device_id_type=MESH
            )
    for c in range(count):
        for d in range(1, replicas):
            load(c, d).start()
    index_copies = [
        pltpu.make_async_copy(block_map_far, block_map, index_sem.at[0]),
        pltpu.make_async_copy(step_offsets_far, step_offsets, index_sem.at[1]),
    ]
    for copy in index_copies:
        copy.start()
    for c in range(count):
        load(c, 0).start()
    states = [
        pltpu.make_async_copy(source, held, state_sem.at[i])
        for i, (source, held) in enumerate(
            ((master_params, master), (first_moment, first), (second_moment, second))
        )
    ]
    for copy in states:
        copy.start()

    def note_order(e, carry):
        seen = jnp.int32(0)
        found = [jnp.int32(0)] * pairs
        for j in range(blocks):
            owned = lax.div(block_map[my_expert * blocks + j], jnp.int32(blocks)) == e
            for k in range(pairs):
                found[k] = jnp.where(owned, jnp.where(seen == k, j, found[k]), found[k])
            seen = seen + jnp.where(owned, 1, 0)
        for k in range(pairs):
            order[e * pairs + k] = found[k]
        return carry

    def note_slots(i, carry):
        seen = jnp.int32(0)
        found = [jnp.int32(0)] * pairs
        for j in range(blocks):
            slot = block_map[i * blocks + j] - my_expert * blocks
            owned = jnp.where(slot >= 0, jnp.where(slot < blocks, 1, 0), 0)
            for k in range(pairs):
                found[k] = jnp.where(owned == 1, jnp.where(seen == k, slot, found[k]), found[k])
            seen = seen + owned
        for k in range(pairs):
            slots[i * pairs + k] = found[k]
        return carry

    def note_places(s, carry):
        place = jnp.int32(0)
        for q in range(blocks):
            place = jnp.where(slots[q] == s, q, place)
        places[s] = place
        return carry

    pl.semaphore_wait(barrier, replicas + experts + tensors - 3)
    for c in range(count):
        for d in range(1, replicas):
            load(c, d).wait()
            y_copy(c, d).start()

    for copy in index_copies:
        copy.wait()
    lax.fori_loop(0, experts, note_order, 0)
    lax.fori_loop(0, experts, note_slots, 0)
    lax.fori_loop(0, blocks, note_places, 0)

    shares = [
        1.0 / jnp.full((8, LANES), 1 + step_offsets[lax.rem(my_replica + replicas - d, replicas)], jnp.int32).astype(jnp.float32)
        for d in range(replicas)
    ]
    total = functools.reduce(lambda a, b: a + b, shares)
    weights = [(share / total)[:1] for share in shares]

    fix_one = 1.0 - beta_one**outer_round
    fix_two = 1.0 - beta_two**outer_round

    def add_up(c):
        load(c, 0).wait()
        all_of(arrived[c], y_recv.at[c]).wait()
        dense = chunks[c] * rows
        own = stage[c].reshape(replicas, blocks, dense, LANES)
        others = arrived[c].reshape(replicas - 1, blocks, dense, LANES)
        out = outgoing[c].reshape(blocks, dense, LANES)

        def step(n, carry):
            for u in range(UNROLL):
                p = n * UNROLL + u
                block = order[p]
                value = own[0, block].astype(jnp.float32) * weights[0]
                for d in range(1, replicas):
                    value = value + others[d - 1, block].astype(jnp.float32) * weights[d]
                out[p] = value.astype(jnp.bfloat16)
            return carry

        lax.fori_loop(0, blocks // UNROLL, step, 0)

    def adam(c):
        dense = chunks[c] * rows
        terms = incoming[c].reshape(blocks, dense, LANES)
        held = params.reshape(blocks, tensors * columns * rows, LANES)
        part = pl.ds(starts[c] * rows, dense)
        target = pl.ds(pl.multiple_of((my_tensor * columns + starts[c]) * rows, 8), dense)

        def step(n, carry):
            for u in range(UNROLL):
                s = n * UNROLL + u
                gradient = terms[places[s]].astype(jnp.float32)
                one = beta_one * first[s, part] + (1.0 - beta_one) * gradient
                two = beta_two * second[s, part] + (1.0 - beta_two) * gradient * gradient
                new_first[s, part] = one
                new_second[s, part] = two
                update = (outer_rate / fix_one) * one / (jnp.sqrt(two * (1.0 / fix_two)) + epsilon)
                held[s, target] = (master[s, part] - update).astype(jnp.bfloat16)
            return carry

        lax.fori_loop(0, blocks // UNROLL, step, 0)

    def finish(c):
        if c == 0:
            for copy in states:
                copy.wait()
        all_of(incoming[c].at[pl.ds(0, (experts - 1) * pairs)], z_recv.at[c]).wait()
        mine = pl.ds(my_expert * pairs, pairs)
        incoming[c][mine] = outgoing[c][mine]
        adam(c)
        for d in range(1, tensors):
            x_copy(c, d).start()

    for c in range(count):
        add_up(c)
        for d in reversed(range(1, experts)):
            z_copy(c, d).start()
        if c >= LAG:
            finish(c - LAG)
    for c in range(max(count - LAG, 0), count):
        finish(c)

    for c in range(count):
        all_of(arrived[c], y_send).wait()
        all_of(incoming[c].at[pl.ds(0, (experts - 1) * pairs)], z_send).wait()
    others = params.at[:, pl.ds(0, (tensors - 1) * columns)]
    all_of(others, x_send).wait()
    all_of(others, x_recv).wait()


def write_out(*refs):
    half = (len(refs) - 1) // 2
    sems = refs[-1]
    copies = [
        pltpu.make_async_copy(refs[i], refs[half + i], sems.at[i])
        for i in range(half)
    ]
    for copy in copies:
        copy.start()
    for copy in copies:
        copy.wait()


def split(columns):
    middle = columns - 2 * EDGE
    return [EDGE] + [CHUNK] * (middle // CHUNK) + [EDGE]


def body(delta, step_offsets, block_map, master_params, first_moment, second_moment, *, shape):
    replicas, experts, tensors = shape
    blocks, rows_all, width = delta.shape[1:]
    rows = rows_all // replicas
    columns = width // LANES
    pairs = blocks // experts
    chunks = split(columns)
    count = len(chunks)
    terms = delta.reshape(blocks, replicas, rows, columns, LANES).transpose(0, 3, 1, 2, 4)

    def dense(state):
        split = state.reshape(blocks, rows, columns, LANES).transpose(0, 2, 1, 3)
        return split.reshape(blocks, columns * rows, LANES)

    def undense(state):
        split = state.reshape(blocks, columns, rows, LANES).transpose(0, 2, 1, 3)
        return split.reshape(blocks, rows, width)

    state_shape = (blocks, columns * rows, LANES)
    params_shape = (blocks, tensors * columns, rows, LANES)
    anywhere = pl.BlockSpec(memory_space=pltpu.HBM)
    near = pl.BlockSpec(memory_space=pltpu.VMEM)
    dma = pltpu.SemaphoreType.DMA
    sizes = (replicas, experts, tensors, chunks, blocks, pairs, rows)
    held = pl.pallas_call(
        functools.partial(kernel, sizes),
        out_shape=(
            pltpu.VMEM(params_shape, jnp.bfloat16),
            pltpu.VMEM(state_shape, jnp.float32),
            pltpu.VMEM(state_shape, jnp.float32),
        ),
        in_specs=[anywhere] * 6,
        out_specs=(near,) * 3,
        scratch_shapes=[
            pltpu.VMEM(state_shape, jnp.float32),
            pltpu.VMEM(state_shape, jnp.float32),
            pltpu.VMEM(state_shape, jnp.float32),
            pltpu.SMEM(block_map.shape, jnp.int32),
            pltpu.SMEM(step_offsets.shape, jnp.int32),
            pltpu.SMEM((blocks,), jnp.int32),
            pltpu.SMEM((blocks,), jnp.int32),
            pltpu.SMEM((blocks,), jnp.int32),
            dma((2,)),
            dma((count, replicas)),
            dma((3,)),
            dma,
            dma((count,)),
            dma,
            dma((count,)),
            dma,
            dma,
        ]
        + [pltpu.VMEM((replicas, blocks, c, rows, LANES), jnp.bfloat16) for c in chunks]
        + [pltpu.VMEM((replicas - 1, blocks, c, rows, LANES), jnp.bfloat16) for c in chunks]
        + [pltpu.VMEM((blocks, c, rows, LANES), jnp.bfloat16) for c in chunks]
        + [pltpu.VMEM((blocks, c, rows, LANES), jnp.bfloat16) for c in chunks],
        compiler_params=pltpu.CompilerParams(collective_id=0, has_side_effects=True),
    )(block_map, step_offsets, terms, dense(master_params), dense(first_moment), dense(second_moment))
    new_params, new_first, new_second = pl.pallas_call(
        write_out,
        out_shape=(
            jax.ShapeDtypeStruct(params_shape, jnp.bfloat16),
            jax.ShapeDtypeStruct(state_shape, jnp.float32),
            jax.ShapeDtypeStruct(state_shape, jnp.float32),
        ),
        in_specs=[near] * 3,
        out_specs=(anywhere,) * 3,
        scratch_shapes=[dma((3,))],
        compiler_params=pltpu.CompilerParams(vmem_limit_bytes=1024 * 1024),
    )(*held)
    full = new_params.transpose(0, 2, 1, 3).reshape(blocks, rows, tensors * width)
    return (full, undense(new_first), undense(new_second))


def solution(mesh):
    in_specs = (
        P("replica", "expert", None, "tensor"),
        P(),
        P(),
        P("expert", "replica", "tensor"),
        P("expert", "replica", "tensor"),
        P("expert", "replica", "tensor"),
    )
    out_specs = (
        P("expert", "replica", None),
        P("expert", "replica", "tensor"),
        P("expert", "replica", "tensor"),
    )
    shape = tuple(mesh.shape[axis] for axis in ("replica", "expert", "tensor"))
    step = functools.partial(body, shape=shape)
    return jax.shard_map(step, mesh=mesh, in_specs=in_specs, out_specs=out_specs, check_vma=False)
```

```python
import functools

import jax
import jax.numpy as jnp
from jax import lax
from jax.experimental import pallas as pl
from jax.experimental.pallas import tpu as pltpu
from jax.sharding import PartitionSpec as P

beta_one = 0.9
beta_two = 0.99
outer_rate = 0.7
outer_round = 20
epsilon = 1e-08

LANES = 128
CHUNK = 4
EDGE = 4
LATE = 8
TURN = 21
EARLY = 99
LAGS = (8, 16, 24)
MESH = pl.DeviceIdType.MESH


def target(mine, d, size):
    if size & (size - 1):
        return lax.rem(mine + d, size)
    if not isinstance(d, int):
        peer = mine
        bit = 1
        while bit < size:
            both = lax.rem(lax.div(mine, bit), 2) * lax.rem(lax.div(d, bit), 2)
            peer = peer + bit * (lax.rem(lax.div(d, bit), 2) - 2 * both)
            bit *= 2
        return peer
    peer = mine
    bit = 1
    while bit < size:
        if d & bit:
            peer = peer + bit * (1 - 2 * lax.rem(lax.div(mine, bit), 2))
        bit *= 2
    return peer


def origin(mine, d, size):
    if size & (size - 1):
        return lax.rem(mine + size - d, size)
    return target(mine, d, size)


def kernel(
    sizes,
    block_map_far,
    step_offsets_far,
    delta,
    master_params,
    first_moment,
    second_moment,
    params,
    new_first,
    new_second,
    state,
    first_held,
    second_held,
    own,
    params_held,
    params_arrived,
    block_map,
    step_offsets,
    order,
    slots,
    places,
    index_sem,
    load_sem,
    own_sem,
    state_sem,
    y_send,
    y_recv,
    z_send,
    z_recv,
    late_recv,
    x_send,
    x_recv,
    *buffers,
):
    replicas, experts, tensors, chunks, late, blocks, pairs, rows = sizes
    count = len(chunks)
    stage = buffers[: count + 1]
    arrived = buffers[count + 1 : 2 * count + 1]
    outgoing = buffers[2 * count + 1 : 3 * count + 1]
    incoming = buffers[3 * count + 1 : 4 * count + 1]
    late_out, late_in, late_arrived = buffers[4 * count + 1 :]
    my_replica = lax.axis_index("replica")
    my_expert = lax.axis_index("expert")
    my_tensor = lax.axis_index("tensor")
    widths = chunks + [late]
    columns = sum(widths)
    starts = [sum(widths[:c]) for c in range(count + 1)]
    groups = [(0, 2), (2, 4), (4, experts)]

    def load(c, d):
        replica = lax.rem(my_replica + d, replicas)
        return pltpu.make_async_copy(
            delta.at[:, pl.ds(starts[c], widths[c]), replica],
            stage[c].at[d - 1],
            load_sem.at[c, d - 1],
        )

    def y_copy(c, d):
        return pltpu.make_async_remote_copy(
            src_ref=late_in.at[:, d] if c == count else stage[c].at[d - 1],
            dst_ref=late_arrived.at[d - 1] if c == count else arrived[c].at[d - 1],
            send_sem=y_send,
            recv_sem=y_recv.at[c],
            device_id={"replica": lax.rem(my_replica + d, replicas)},
            device_id_type=MESH,
        )

    def z_copy(c, d):
        part = pl.ds(d * pairs, pairs)
        return pltpu.make_async_remote_copy(
            src_ref=late_out.at[d] if c == count else outgoing[c].at[part],
            dst_ref=late_in.at[d] if c == count else incoming[c].at[part],
            send_sem=z_send,
            recv_sem=late_recv if c == count else z_recv.at[c, group_of(d)],
            device_id={"expert": target(my_expert, d, experts)},
            device_id_type=MESH,
        )

    def group_of(d):
        return [g for g, (low, high) in enumerate(groups) if low <= d < high][0]

    def x_copy(c, low, high, d):
        part = (pl.ds(low * pairs, (high - low) * pairs), pl.ds(starts[c], widths[c]))
        return pltpu.make_async_remote_copy(
            src_ref=params_held.at[part],
            dst_ref=params_arrived.at[(d - 1,) + part],
            send_sem=x_send,
            recv_sem=x_recv,
            device_id={"tensor": lax.rem(my_tensor + d, tensors)},
            device_id_type=MESH,
        )

    def all_of(ref, sem):
        return pltpu.make_async_copy(ref, ref, sem)

    barrier = pltpu.get_barrier_semaphore()
    axes = (("expert", my_expert, experts), ("replica", my_replica, replicas), ("tensor", my_tensor, tensors))
    for axis, mine, size in axes:
        for d in reversed(range(1, size)):
            pl.semaphore_signal(
                barrier, inc=1, device_id={axis: lax.rem(mine + d, size)}, device_id_type=MESH
            )
    for c in range(count + 1):
        for d in range(1, replicas):
            load(c, d).start()
    index_copies = [
        pltpu.make_async_copy(block_map_far, block_map, index_sem.at[0]),
        pltpu.make_async_copy(step_offsets_far, step_offsets, index_sem.at[1]),
    ]
    for copy in index_copies:
        copy.start()
    own_load = pltpu.make_async_copy(delta.at[:, :, my_replica], own, own_sem)
    own_load.start()
    for i, source in enumerate((master_params, first_moment, second_moment)):
        pltpu.make_async_copy(source, state.at[i], state_sem).start()

    def digits(key, k):
        return jnp.maximum(lax.rem(lax.div(key, jnp.int32(blocks ** (pairs - 1 - k))), jnp.int32(blocks)), 0)

    def note_order(d, carry):
        low = target(my_expert, d, experts) * blocks
        key = jnp.int32(0)
        for j in range(blocks):
            slot = block_map[my_expert * blocks + j] - low
            owned = jnp.where(slot >= 0, slot, blocks) < blocks
            key = jnp.where(owned, key * blocks + j, key)
        for k in range(pairs):
            order[d * pairs + k] = digits(key, k)
        return carry

    def note_slots(d, carry):
        low = origin(my_expert, d, experts) * blocks
        key = jnp.int32(0)
        for j in range(blocks):
            slot = block_map[low + j] - my_expert * blocks
            owned = jnp.where(slot >= 0, slot, blocks) < blocks
            key = jnp.where(owned, key * blocks + slot, key)
        for k in range(pairs):
            slots[d * pairs + k] = digits(key, k)
        return carry

    def note_places(s, carry):
        place = jnp.int32(0)
        for q in range(blocks):
            place = jnp.where(slots[q] == s, q, place)
        places[s] = place
        return carry

    pl.semaphore_wait(barrier, replicas + experts + tensors - 3)
    early = min(EARLY, count)
    for c in range(early):
        for d in range(1, replicas):
            load(c, d).wait()
            y_copy(c, d).start()

    for copy in index_copies:
        copy.wait()
    lax.fori_loop(0, experts, note_order, 0)

    own_load.wait()
    for c in range(early, count + 1):
        for d in range(1, replicas):
            load(c, d).wait()
    late_dense = late * rows
    for d in range(experts):
        held = (late_in if d == 0 else late_out).reshape(experts, replicas, pairs, late_dense, LANES)
        own_flat = own.reshape(blocks, columns * rows, LANES)
        rest = stage[count].reshape(replicas - 1, blocks, late_dense, LANES)
        for k in range(pairs):
            block = order[d * pairs + k]
            held[d, 0, k] = own_flat[block, pl.ds(starts[count] * rows, late_dense)]
            for r in range(1, replicas):
                held[d, r, k] = rest[r - 1, block]
    for d in reversed(range(1, experts)):
        z_copy(count, d).start()

    lax.fori_loop(0, experts, note_slots, 0)
    lax.fori_loop(0, blocks, note_places, 0)

    shares = [
        1.0 / jnp.full((8, LANES), 1 + step_offsets[lax.rem(my_replica + replicas - d, replicas)], jnp.int32).astype(jnp.float32)
        for d in range(replicas)
    ]
    total = functools.reduce(lambda a, b: a + b, shares)
    weights = [(share / total)[:1] for share in shares]

    fix_one = 1.0 - beta_one**outer_round
    fix_two = 1.0 - beta_two**outer_round

    def add_up(c):
        all_of(arrived[c], y_recv.at[c]).wait()
        dense = chunks[c] * rows
        part = pl.ds(starts[c] * rows, dense)
        own_flat = own.reshape(blocks, columns * rows, LANES)
        others = arrived[c].reshape(replicas - 1, blocks, dense, LANES)
        out = outgoing[c].reshape(blocks, dense, LANES)
        for q in range(blocks):
            block = order[q]
            value = own_flat[block, part].astype(jnp.float32) * weights[0]
            for d in range(1, replicas):
                value = value + others[d - 1, block].astype(jnp.float32) * weights[d]
            out[q] = value.astype(jnp.bfloat16)

    def adam(c, q, gradient):
        part = pl.ds(starts[c] * rows, widths[c] * rows)
        slot = slots[q]
        one = beta_one * state[1, slot, part] + (1.0 - beta_one) * gradient
        two = beta_two * state[2, slot, part] + (1.0 - beta_two) * gradient * gradient
        first_held[q, part] = one
        second_held[q, part] = two
        update = (outer_rate / fix_one) * one / (jnp.sqrt(two * (1.0 / fix_two)) + epsilon)
        held = params_held.reshape(blocks, columns * rows, LANES)
        held[q, part] = (state[0, slot, part] - update).astype(jnp.bfloat16)

    def finish(c, g):
        if c == 0 and g == 0:
            all_of(state, state_sem).wait()
        low, high = groups[g]
        got = (max(low, 1) * pairs, high * pairs)
        all_of(incoming[c].at[pl.ds(got[0], got[1] - got[0])], z_recv.at[c, g]).wait()
        dense = chunks[c] * rows
        for q in range(low * pairs, high * pairs):
            terms = (outgoing[c] if q < pairs else incoming[c]).reshape(blocks, dense, LANES)
            adam(c, q, terms[q].astype(jnp.float32))
        for d in range(1, tensors):
            x_copy(c, low, high, d).start()

    def finish_late():
        all_of(late_arrived, y_recv.at[count]).wait()
        mine = late_in.reshape(experts, replicas, pairs, late_dense, LANES)
        others = late_arrived.reshape(replicas - 1, experts, pairs, late_dense, LANES)
        for q in range(blocks):
            e, k = divmod(q, pairs)
            value = mine[e, 0, k].astype(jnp.float32) * weights[0]
            for d in range(1, replicas):
                value = value + others[d - 1, e, k].astype(jnp.float32) * weights[d]
            adam(count, q, value)
        for d in range(1, tensors):
            x_copy(count, 0, experts, d).start()

    def settle(c):
        part = pl.ds(starts[c] * rows, widths[c] * rows)
        goal = pl.ds(pl.multiple_of((my_tensor * columns + starts[c]) * rows, 8), widths[c] * rows)
        flat = params.reshape(blocks, tensors * columns * rows, LANES)
        held = params_held.reshape(blocks, columns * rows, LANES)
        for s in range(blocks):
            place = places[s]
            new_first[s, part] = first_held[place, part]
            new_second[s, part] = second_held[place, part]
            flat[s, goal] = held[place, part]

    def add_and_send(c):
        add_up(c)
        for d in reversed(range(1, experts)):
            z_copy(c, d).start()

    def turn():
        all_of(late_in.at[pl.ds(1, experts - 1)], late_recv).wait()
        for c in [count] + list(range(early, count)):
            for d in range(1, replicas):
                y_copy(c, d).start()

    def last(c):
        finish(c, 2)
        settle(c)

    def whole_late():
        finish_late()
        settle(count)

    steps = [(TURN, 0, turn)]
    landed = 0
    for c in list(range(early)) + [count] + list(range(early, count)):
        landed += widths[c]
        if c == count:
            steps.append((landed, 2, whole_late))
            continue
        steps.append((landed, 1, functools.partial(add_and_send, c)))
        steps.append((landed + LAGS[0], 3, functools.partial(finish, c, 0)))
        steps.append((landed + LAGS[1], 4, functools.partial(finish, c, 1)))
        steps.append((landed + LAGS[2], 5, functools.partial(last, c)))
    for _, _, step in sorted(steps, key=lambda entry: entry[:2]):
        step()

    for c in range(count):
        all_of(arrived[c], y_send).wait()
        all_of(incoming[c].at[pl.ds(0, (experts - 1) * pairs)], z_send).wait()
    all_of(late_arrived, y_send).wait()
    all_of(late_in.at[pl.ds(1, experts - 1)], z_send).wait()
    all_of(params_arrived, x_send).wait()
    all_of(params_arrived, x_recv).wait()
    flat = params.reshape(blocks, tensors * columns * rows, LANES)
    others = params_arrived.reshape(tensors - 1, blocks, columns * rows, LANES)
    for d in range(1, tensors):
        sender = lax.rem(my_tensor + tensors - d, tensors)
        goal = pl.ds(pl.multiple_of(sender * columns * rows, 8), columns * rows)
        for s in range(blocks):
            flat[s, goal] = others[d - 1, places[s]]


def write_out(*refs):
    half = (len(refs) - 1) // 2
    sems = refs[-1]
    copies = [
        pltpu.make_async_copy(refs[i], refs[half + i], sems.at[i])
        for i in range(half)
    ]
    for copy in copies:
        copy.start()
    for copy in copies:
        copy.wait()


def split(columns):
    late = LATE
    middle = columns - late - 2 * EDGE
    return [EDGE] + [CHUNK] * (middle // CHUNK) + [EDGE] * (1 + middle % CHUNK // EDGE), late


def body(delta, step_offsets, block_map, master_params, first_moment, second_moment, *, shape):
    replicas, experts, tensors = shape
    blocks, rows_all, width = delta.shape[1:]
    rows = rows_all // replicas
    columns = width // LANES
    pairs = blocks // experts
    chunks, late = split(columns)
    count = len(chunks)
    terms = delta.reshape(blocks, replicas, rows, columns, LANES).transpose(0, 3, 1, 2, 4)

    def dense(state):
        split = state.reshape(blocks, rows, columns, LANES).transpose(0, 2, 1, 3)
        return split.reshape(blocks, columns * rows, LANES)

    def undense(state):
        split = state.reshape(blocks, columns, rows, LANES).transpose(0, 2, 1, 3)
        return split.reshape(blocks, rows, width)

    state_shape = (blocks, columns * rows, LANES)
    params_shape = (blocks, tensors * columns, rows, LANES)
    anywhere = pl.BlockSpec(memory_space=pltpu.HBM)
    near = pl.BlockSpec(memory_space=pltpu.VMEM)
    dma = pltpu.SemaphoreType.DMA
    sizes = (replicas, experts, tensors, chunks, late, blocks, pairs, rows)
    piece = (rows, LANES)
    held = pl.pallas_call(
        functools.partial(kernel, sizes),
        out_shape=(
            pltpu.VMEM(params_shape, jnp.bfloat16),
            pltpu.VMEM(state_shape, jnp.float32),
            pltpu.VMEM(state_shape, jnp.float32),
        ),
        in_specs=[anywhere] * 6,
        out_specs=(near,) * 3,
        scratch_shapes=[
            pltpu.VMEM((3,) + state_shape, jnp.float32),
            pltpu.VMEM(state_shape, jnp.float32),
            pltpu.VMEM(state_shape, jnp.float32),
            pltpu.VMEM((blocks, columns) + piece, jnp.bfloat16),
            pltpu.VMEM((blocks, columns) + piece, jnp.bfloat16),
            pltpu.VMEM((tensors - 1, blocks, columns) + piece, jnp.bfloat16),
            pltpu.SMEM(block_map.shape, jnp.int32),
            pltpu.SMEM(step_offsets.shape, jnp.int32),
            pltpu.SMEM((blocks,), jnp.int32),
            pltpu.SMEM((blocks,), jnp.int32),
            pltpu.SMEM((blocks,), jnp.int32),
            dma((2,)),
            dma((count + 1, replicas - 1)),
            dma,
            dma,
            dma,
            dma((count + 1,)),
            dma,
            dma((count, 3)),
            dma,
            dma,
            dma,
        ]
        + [pltpu.VMEM((replicas - 1, blocks, c) + piece, jnp.bfloat16) for c in chunks + [late]]
        + [pltpu.VMEM((replicas - 1, blocks, c) + piece, jnp.bfloat16) for c in chunks]
        + [pltpu.VMEM((blocks, c) + piece, jnp.bfloat16) for c in chunks]
        + [pltpu.VMEM((blocks, c) + piece, jnp.bfloat16) for c in chunks]
        + [pltpu.VMEM((experts, replicas, pairs, late) + piece, jnp.bfloat16)] * 2
        + [pltpu.VMEM((replicas - 1, experts, pairs, late) + piece, jnp.bfloat16)],
        compiler_params=pltpu.CompilerParams(collective_id=0, has_side_effects=True),
    )(block_map, step_offsets, terms, dense(master_params), dense(first_moment), dense(second_moment))
    new_params, new_first, new_second = pl.pallas_call(
        write_out,
        out_shape=(
            jax.ShapeDtypeStruct(params_shape, jnp.bfloat16),
            jax.ShapeDtypeStruct(state_shape, jnp.float32),
            jax.ShapeDtypeStruct(state_shape, jnp.float32),
        ),
        in_specs=[near] * 3,
        out_specs=(anywhere,) * 3,
        scratch_shapes=[dma((3,))],
        compiler_params=pltpu.CompilerParams(vmem_limit_bytes=1024 * 1024),
    )(*held)
    full = new_params.transpose(0, 2, 1, 3).reshape(blocks, rows, tensors * width)
    return (full, undense(new_first), undense(new_second))


def solution(mesh):
    in_specs = (
        P("replica", "expert", None, "tensor"),
        P(),
        P(),
        P("expert", "replica", "tensor"),
        P("expert", "replica", "tensor"),
        P("expert", "replica", "tensor"),
    )
    out_specs = (
        P("expert", "replica", None),
        P("expert", "replica", "tensor"),
        P("expert", "replica", "tensor"),
    )
    shape = tuple(mesh.shape[axis] for axis in ("replica", "expert", "tensor"))
    step = functools.partial(body, shape=shape)
    return jax.shard_map(step, mesh=mesh, in_specs=in_specs, out_specs=out_specs, check_vma=False)
```

```python
import functools

import jax
import jax.numpy as jnp
from jax import lax
from jax.experimental import pallas as pl
from jax.experimental.pallas import tpu as pltpu
from jax.sharding import PartitionSpec as P

beta_one = 0.9
beta_two = 0.99
outer_rate = 0.7
outer_round = 20
epsilon = 1e-08

LANES = 128
CHUNK = 4
EDGE = 4
LATE = 8
SORTS = (4, 4)
REST = (11, 13)
AHEAD = 7
TURN = 21
LAGS = (8, 16, 24)
FIRST_LAGS = (8, 16, 24)
MESH = pl.DeviceIdType.MESH


def target(mine, d, size):
    if size & (size - 1):
        return lax.rem(mine + d, size)
    if not isinstance(d, int):
        peer = mine
        bit = 1
        while bit < size:
            both = lax.rem(lax.div(mine, bit), 2) * lax.rem(lax.div(d, bit), 2)
            peer = peer + bit * (lax.rem(lax.div(d, bit), 2) - 2 * both)
            bit *= 2
        return peer
    peer = mine
    bit = 1
    while bit < size:
        if d & bit:
            peer = peer + bit * (1 - 2 * lax.rem(lax.div(mine, bit), 2))
        bit *= 2
    return peer


def between(mine, peer, size):
    if size & (size - 1):
        return lax.rem(peer + size - mine, size)
    return target(mine, peer, size)


def origin(mine, d, size):
    if size & (size - 1):
        return lax.rem(mine + size - d, size)
    return target(mine, d, size)


def kernel(
    sizes,
    block_map_far,
    step_offsets_far,
    delta,
    master_params,
    first_moment,
    second_moment,
    params,
    new_first,
    new_second,
    state,
    first_held,
    second_held,
    own,
    params_held,
    params_arrived,
    block_map,
    step_offsets,
    order,
    slots,
    places,
    index_sem,
    load_sem,
    own_sem,
    state_sem,
    y_send,
    y_recv,
    z_send,
    z_recv,
    late_recv,
    x_send,
    x_recv,
    *buffers,
):
    replicas, experts, tensors, chunks, sorts, late, blocks, pairs, rows = sizes
    widths = chunks + sorts + [late]
    plain = len(chunks)
    count = len(widths) - 1
    raw = buffers[0]
    arrived = buffers[1 : count + 1]
    outgoing = buffers[count + 1 : 2 * count + 1]
    incoming = buffers[2 * count + 1 : 3 * count + 1]
    staged = buffers[3 * count + 1 : -3]
    late_out, late_in, late_arrived = buffers[-3:]
    my_replica = lax.axis_index("replica")
    my_expert = lax.axis_index("expert")
    my_tensor = lax.axis_index("tensor")
    columns = sum(widths)
    starts = [sum(widths[:c]) for c in range(count + 1)]
    groups = [(0, 2), (2, 4), (4, experts)]

    halves = [(0, 2 * pairs), (2 * pairs, blocks)]

    def load(n, d):
        replica = lax.rem(my_replica + d, replicas)
        part = pl.ds(0, chunks[0]) if n == 0 else pl.ds(chunks[0], columns - chunks[0])
        return pltpu.make_async_copy(
            delta.at[:, part, replica],
            raw.at[d - 1, :, part],
            load_sem.at[n, d - 1],
        )

    def arrival(c, h):
        return c + h + max(c - plain, 0)

    def y_copy(c, h, d):
        low, high = halves[h]
        if c == count:
            source, goal = late_in.at[:, d], late_arrived.at[d - 1]
        elif c < plain:
            source, goal = raw.at[d - 1, :, pl.ds(starts[c], widths[c])], arrived[c].at[d - 1]
        else:
            part = (d - 1, pl.ds(low, high - low))
            source, goal = staged[c - plain].at[part], arrived[c].at[part]
        return pltpu.make_async_remote_copy(
            src_ref=source,
            dst_ref=goal,
            send_sem=y_send,
            recv_sem=y_recv.at[arrival(c, h)],
            device_id={"replica": lax.rem(my_replica + d, replicas)},
            device_id_type=MESH,
        )

    def z_copy(c, d):
        part = pl.ds(d * pairs, pairs)
        return pltpu.make_async_remote_copy(
            src_ref=late_out.at[d] if c == count else outgoing[c].at[part],
            dst_ref=late_in.at[d] if c == count else incoming[c].at[part],
            send_sem=z_send,
            recv_sem=late_recv if c == count else z_recv.at[c, group_of(d)],
            device_id={"expert": target(my_expert, d, experts)},
            device_id_type=MESH,
        )

    def sorted_copy(c, e):
        d = between(my_expert, e, experts)
        return pltpu.make_async_remote_copy(
            src_ref=outgoing[c].at[pl.ds(e * pairs, pairs)],
            dst_ref=incoming[c].at[pl.ds(d * pairs, pairs)],
            send_sem=z_send,
            recv_sem=z_recv.at[c, jnp.minimum(lax.div(d, 2), 2)],
            device_id={"expert": e},
            device_id_type=MESH,
        )

    def group_of(d):
        return [g for g, (low, high) in enumerate(groups) if low <= d < high][0]

    def x_copy(c, low, high, d):
        part = (pl.ds(low * pairs, (high - low) * pairs), pl.ds(starts[c], widths[c]))
        return pltpu.make_async_remote_copy(
            src_ref=params_held.at[part],
            dst_ref=params_arrived.at[(d - 1,) + part],
            send_sem=x_send,
            recv_sem=x_recv,
            device_id={"tensor": lax.rem(my_tensor + d, tensors)},
            device_id_type=MESH,
        )

    def all_of(ref, sem):
        return pltpu.make_async_copy(ref, ref, sem)

    barrier = pltpu.get_barrier_semaphore()
    axes = (("expert", my_expert, experts), ("replica", my_replica, replicas), ("tensor", my_tensor, tensors))
    for axis, mine, size in axes:
        for d in reversed(range(1, size)):
            pl.semaphore_signal(
                barrier, inc=1, device_id={axis: lax.rem(mine + d, size)}, device_id_type=MESH
            )
    for n in range(2):
        for d in range(1, replicas):
            load(n, d).start()
    index_copies = [
        pltpu.make_async_copy(block_map_far, block_map, index_sem.at[0]),
        pltpu.make_async_copy(step_offsets_far, step_offsets, index_sem.at[1]),
    ]
    for copy in index_copies:
        copy.start()
    own_load = pltpu.make_async_copy(delta.at[:, :, my_replica], own, own_sem)
    own_load.start()
    for i, source in enumerate((master_params, first_moment, second_moment)):
        pltpu.make_async_copy(source, state.at[i], state_sem).start()

    def digits(key, k):
        return jnp.maximum(lax.rem(lax.div(key, jnp.int32(blocks ** (pairs - 1 - k))), jnp.int32(blocks)), 0)

    def note_order():
        owners = [lax.div(block_map[my_expert * blocks + j], jnp.int32(blocks)) for j in range(blocks)]
        for d in range(experts):
            wanted = target(my_expert, d, experts)
            key = jnp.int32(0)
            for j in range(blocks):
                key = jnp.where(owners[j] == wanted, key * blocks + j, key)
            for k in range(pairs):
                order[d * pairs + k] = digits(key, k)

    def note_slots(d, carry):
        low = origin(my_expert, d, experts) * blocks
        key = jnp.int32(0)
        for j in range(blocks):
            slot = block_map[low + j] - my_expert * blocks
            owned = jnp.where(slot >= 0, slot, blocks) < blocks
            key = jnp.where(owned, key * blocks + slot, key)
        for k in range(pairs):
            slots[d * pairs + k] = digits(key, k)
        return carry

    def note_places(s, carry):
        place = jnp.int32(0)
        for q in range(blocks):
            place = jnp.where(slots[q] == s, q, place)
        places[s] = place
        return carry

    pl.semaphore_wait(barrier, replicas + experts + tensors - 3)
    for d in range(1, replicas):
        load(0, d).wait()
        y_copy(0, 0, d).start()

    for copy in index_copies:
        copy.wait()
    note_order()

    def block_of(j):
        return order[between(my_expert, j // pairs, experts) * pairs + j % pairs]

    def gather(c, h):
        dense = widths[c] * rows
        far = raw.reshape(replicas - 1, blocks, columns * rows, LANES)
        goal = staged[c - plain].reshape(replicas - 1, blocks, dense, LANES)
        for j in range(*halves[h]):
            for r in range(1, replicas):
                goal[r - 1, j] = far[r - 1, block_of(j), pl.ds(starts[c] * rows, dense)]

    stream = [(0, 0)] + [(c, 0) for c in range(plain, count)] + [(c, 0) for c in range(1, plain)]
    for c in range(plain, count):
        stream.insert(min(REST[c - plain], len(stream)), (c, 1))

    def send(part):
        for c, h in part:
            if c >= plain:
                gather(c, h)
            for d in range(1, replicas):
                y_copy(c, h, d).start()

    for d in range(1, replicas):
        load(1, d).wait()
    send(stream[1:AHEAD])

    own_load.wait()
    late_dense = late * rows
    for d in range(experts):
        held = (late_in if d == 0 else late_out).reshape(experts, replicas, pairs, late_dense, LANES)
        own_flat = own.reshape(blocks, columns * rows, LANES)
        rest = raw.reshape(replicas - 1, blocks, columns * rows, LANES)
        for k in range(pairs):
            block = order[d * pairs + k]
            held[d, 0, k] = own_flat[block, pl.ds(starts[count] * rows, late_dense)]
            for r in range(1, replicas):
                held[d, r, k] = rest[r - 1, block, pl.ds(starts[count] * rows, late_dense)]
    for d in reversed(range(1, experts)):
        z_copy(count, d).start()
    send(stream[AHEAD:])

    lax.fori_loop(0, experts, note_slots, 0)
    lax.fori_loop(0, blocks, note_places, 0)

    shares = [
        1.0 / jnp.full((8, LANES), 1 + step_offsets[lax.rem(my_replica + replicas - d, replicas)], jnp.int32).astype(jnp.float32)
        for d in range(replicas)
    ]
    total = functools.reduce(lambda a, b: a + b, shares)
    weights = [(share / total)[:1] for share in shares]

    fix_one = 1.0 - beta_one**outer_round
    fix_two = 1.0 - beta_two**outer_round

    def add_up(c, h):
        low, high = halves[h] if c >= plain else (0, blocks)
        got = arrived[c].at[:, pl.ds(low, high - low)]
        all_of(got, y_recv.at[arrival(c, h)]).wait()
        dense = widths[c] * rows
        part = pl.ds(starts[c] * rows, dense)
        own_flat = own.reshape(blocks, columns * rows, LANES)
        others = arrived[c].reshape(replicas - 1, blocks, dense, LANES)
        out = outgoing[c].reshape(blocks, dense, LANES)
        for q in range(low, high):
            block = block_of(q) if c >= plain else order[q]
            value = own_flat[block, part].astype(jnp.float32) * weights[0]
            for d in range(1, replicas):
                value = value + others[d - 1, q if c >= plain else block].astype(jnp.float32) * weights[d]
            out[q] = value.astype(jnp.bfloat16)

    def adam(c, q, gradient):
        part = pl.ds(starts[c] * rows, widths[c] * rows)
        slot = slots[q]
        one = beta_one * state[1, slot, part] + (1.0 - beta_one) * gradient
        two = beta_two * state[2, slot, part] + (1.0 - beta_two) * gradient * gradient
        first_held[q, part] = one
        second_held[q, part] = two
        update = (outer_rate / fix_one) * one / (jnp.sqrt(two * (1.0 / fix_two)) + epsilon)
        held = params_held.reshape(blocks, columns * rows, LANES)
        held[q, part] = (state[0, slot, part] - update).astype(jnp.bfloat16)

    def finish(c, g):
        low, high = groups[g]
        got = (max(low, 1) * pairs, high * pairs)
        all_of(incoming[c].at[pl.ds(got[0], got[1] - got[0])], z_recv.at[c, g]).wait()
        dense = widths[c] * rows
        for q in range(low * pairs, high * pairs):
            terms = (outgoing[c] if q < pairs else incoming[c]).reshape(blocks, dense, LANES)
            place = my_expert * pairs + q if q < pairs and c >= plain else q
            adam(c, q, terms[place].astype(jnp.float32))
        for d in range(1, tensors):
            x_copy(c, low, high, d).start()

    def finish_late():
        all_of(late_arrived, y_recv.at[arrival(count, 0)]).wait()
        mine = late_in.reshape(experts, replicas, pairs, late_dense, LANES)
        others = late_arrived.reshape(replicas - 1, experts, pairs, late_dense, LANES)
        for q in range(blocks):
            e, k = divmod(q, pairs)
            value = mine[e, 0, k].astype(jnp.float32) * weights[0]
            for d in range(1, replicas):
                value = value + others[d - 1, e, k].astype(jnp.float32) * weights[d]
            adam(count, q, value)
        for d in range(1, tensors):
            x_copy(count, 0, experts, d).start()

    def settle(c):
        part = pl.ds(starts[c] * rows, widths[c] * rows)
        goal = pl.ds(pl.multiple_of((my_tensor * columns + starts[c]) * rows, 8), widths[c] * rows)
        flat = params.reshape(blocks, tensors * columns * rows, LANES)
        held = params_held.reshape(blocks, columns * rows, LANES)
        for s in range(blocks):
            place = places[s]
            new_first[s, part] = first_held[place, part]
            new_second[s, part] = second_held[place, part]
            flat[s, goal] = held[place, part]

    def add_and_send(c, h):
        add_up(c, h)
        if c < plain:
            for d in reversed(range(1, experts)):
                z_copy(c, d).start()
            return
        for e in range(halves[h][0] // pairs, halves[h][1] // pairs):
            pl.when(my_expert != e)(sorted_copy(c, e).start)

    def turn():
        all_of(late_in.at[pl.ds(1, experts - 1)], late_recv).wait()
        for d in range(1, replicas):
            y_copy(count, 0, d).start()

    def ready(c, h, g):
        def act():
            finish(c, g)
            if g == 2:
                settle(c)

        if c < plain:
            act()
        else:
            pl.when(my_expert < 2 if h == 0 else my_expert >= 2)(act)

    def whole_late():
        finish_late()
        settle(count)

    steps = [(TURN, 0, turn)]
    landed = 0
    for c, h in stream:
        landed += widths[c] * (halves[h][1] - halves[h][0]) // blocks if c >= plain else widths[c]
        steps.append((landed, 1, functools.partial(add_and_send, c, h)))
        for g in range(3):
            lag = FIRST_LAGS[g] if c >= plain and h == 0 else LAGS[g]
            steps.append((landed + lag, 3 + g, functools.partial(ready, c, h, g)))
    steps.append((landed + late, 2, whole_late))
    all_of(state, state_sem).wait()
    for _, _, step in sorted(steps, key=lambda entry: entry[:2]):
        step()

    for c in range(count):
        all_of(arrived[c], y_send).wait()
        all_of(incoming[c].at[pl.ds(0, (experts - 1) * pairs)], z_send).wait()
    all_of(late_arrived, y_send).wait()
    all_of(late_in.at[pl.ds(1, experts - 1)], z_send).wait()
    all_of(params_arrived, x_send).wait()
    all_of(params_arrived, x_recv).wait()
    flat = params.reshape(blocks, tensors * columns * rows, LANES)
    others = params_arrived.reshape(tensors - 1, blocks, columns * rows, LANES)
    for d in range(1, tensors):
        sender = lax.rem(my_tensor + tensors - d, tensors)
        goal = pl.ds(pl.multiple_of(sender * columns * rows, 8), columns * rows)
        for s in range(blocks):
            flat[s, goal] = others[d - 1, places[s]]


def write_out(*refs):
    half = (len(refs) - 1) // 2
    sems = refs[-1]
    copies = [
        pltpu.make_async_copy(refs[i], refs[half + i], sems.at[i])
        for i in range(half)
    ]
    for copy in copies:
        copy.start()
    for copy in copies:
        copy.wait()


def split(columns):
    middle = columns - LATE - sum(SORTS) - EDGE
    return [EDGE] + [CHUNK] * (middle // CHUNK), list(SORTS), LATE


def body(delta, step_offsets, block_map, master_params, first_moment, second_moment, *, shape):
    replicas, experts, tensors = shape
    blocks, rows_all, width = delta.shape[1:]
    rows = rows_all // replicas
    columns = width // LANES
    pairs = blocks // experts
    chunks, sorts, late = split(columns)
    widths = chunks + sorts
    count = len(widths)
    terms = delta.reshape(blocks, replicas, rows, columns, LANES).transpose(0, 3, 1, 2, 4)

    def dense(state):
        split = state.reshape(blocks, rows, columns, LANES).transpose(0, 2, 1, 3)
        return split.reshape(blocks, columns * rows, LANES)

    def undense(state):
        split = state.reshape(blocks, columns, rows, LANES).transpose(0, 2, 1, 3)
        return split.reshape(blocks, rows, width)

    state_shape = (blocks, columns * rows, LANES)
    params_shape = (blocks, tensors * columns, rows, LANES)
    anywhere = pl.BlockSpec(memory_space=pltpu.HBM)
    near = pl.BlockSpec(memory_space=pltpu.VMEM)
    dma = pltpu.SemaphoreType.DMA
    sizes = (replicas, experts, tensors, chunks, sorts, late, blocks, pairs, rows)
    piece = (rows, LANES)
    held = pl.pallas_call(
        functools.partial(kernel, sizes),
        out_shape=(
            pltpu.VMEM(params_shape, jnp.bfloat16),
            pltpu.VMEM(state_shape, jnp.float32),
            pltpu.VMEM(state_shape, jnp.float32),
        ),
        in_specs=[anywhere] * 6,
        out_specs=(near,) * 3,
        scratch_shapes=[
            pltpu.VMEM((3,) + state_shape, jnp.float32),
            pltpu.VMEM(state_shape, jnp.float32),
            pltpu.VMEM(state_shape, jnp.float32),
            pltpu.VMEM((blocks, columns) + piece, jnp.bfloat16),
            pltpu.VMEM((blocks, columns) + piece, jnp.bfloat16),
            pltpu.VMEM((tensors - 1, blocks, columns) + piece, jnp.bfloat16),
            pltpu.SMEM(block_map.shape, jnp.int32),
            pltpu.SMEM(step_offsets.shape, jnp.int32),
            pltpu.SMEM((blocks,), jnp.int32),
            pltpu.SMEM((blocks,), jnp.int32),
            pltpu.SMEM((blocks,), jnp.int32),
            dma((2,)),
            dma((2, replicas - 1)),
            dma,
            dma,
            dma,
            dma((count + len(sorts) + 1,)),
            dma,
            dma((count, 3)),
            dma,
            dma,
            dma,
        ]
        + [pltpu.VMEM((replicas - 1, blocks, columns) + piece, jnp.bfloat16)]
        + [pltpu.VMEM((replicas - 1, blocks, c) + piece, jnp.bfloat16) for c in widths]
        + [pltpu.VMEM((blocks, c) + piece, jnp.bfloat16) for c in widths] * 2
        + [pltpu.VMEM((replicas - 1, blocks, c) + piece, jnp.bfloat16) for c in sorts]
        + [pltpu.VMEM((experts, replicas, pairs, late) + piece, jnp.bfloat16)] * 2
        + [pltpu.VMEM((replicas - 1, experts, pairs, late) + piece, jnp.bfloat16)],
        compiler_params=pltpu.CompilerParams(collective_id=0, has_side_effects=True),
    )(block_map, step_offsets, terms, dense(master_params), dense(first_moment), dense(second_moment))
    new_params, new_first, new_second = pl.pallas_call(
        write_out,
        out_shape=(
            jax.ShapeDtypeStruct(params_shape, jnp.bfloat16),
            jax.ShapeDtypeStruct(state_shape, jnp.float32),
            jax.ShapeDtypeStruct(state_shape, jnp.float32),
        ),
        in_specs=[near] * 3,
        out_specs=(anywhere,) * 3,
        scratch_shapes=[dma((3,))],
        compiler_params=pltpu.CompilerParams(vmem_limit_bytes=1024 * 1024),
    )(*held)
    full = new_params.transpose(0, 2, 1, 3).reshape(blocks, rows, tensors * width)
    return (full, undense(new_first), undense(new_second))


def solution(mesh):
    in_specs = (
        P("replica", "expert", None, "tensor"),
        P(),
        P(),
        P("expert", "replica", "tensor"),
        P("expert", "replica", "tensor"),
        P("expert", "replica", "tensor"),
    )
    out_specs = (
        P("expert", "replica", None),
        P("expert", "replica", "tensor"),
        P("expert", "replica", "tensor"),
    )
    shape = tuple(mesh.shape[axis] for axis in ("replica", "expert", "tensor"))
    step = functools.partial(body, shape=shape)
    return jax.shard_map(step, mesh=mesh, in_specs=in_specs, out_specs=out_specs, check_vma=False)
```

```python
import functools

import jax
import jax.numpy as jnp
from jax import lax
from jax.experimental import pallas as pl
from jax.experimental.pallas import tpu as pltpu
from jax.sharding import PartitionSpec as P

beta_one = 0.9
beta_two = 0.99
outer_rate = 0.7
outer_round = 20
epsilon = 1e-08

LANES = 128
CHUNK = 4
LATE = 8
SORTS = (4, 4)
AHEAD = 7
TURN = 21
LAGS = (8, 16, 24)
MESH = pl.DeviceIdType.MESH


def target(mine, d, size):
    if size & (size - 1):
        return lax.rem(mine + d, size)
    if not isinstance(d, int):
        peer = mine
        bit = 1
        while bit < size:
            both = lax.rem(lax.div(mine, bit), 2) * lax.rem(lax.div(d, bit), 2)
            peer = peer + bit * (lax.rem(lax.div(d, bit), 2) - 2 * both)
            bit *= 2
        return peer
    peer = mine
    bit = 1
    while bit < size:
        if d & bit:
            peer = peer + bit * (1 - 2 * lax.rem(lax.div(mine, bit), 2))
        bit *= 2
    return peer


def between(mine, peer, size):
    if size & (size - 1):
        return lax.rem(peer + size - mine, size)
    return target(mine, peer, size)


def origin(mine, d, size):
    if size & (size - 1):
        return lax.rem(mine + size - d, size)
    return target(mine, d, size)


def kernel(
    sizes,
    block_map_far,
    step_offsets_far,
    delta,
    master_params,
    first_moment,
    second_moment,
    params,
    new_first,
    new_second,
    state,
    first_held,
    second_held,
    own,
    params_held,
    params_arrived,
    block_map,
    step_offsets,
    order,
    slots,
    places,
    index_sem,
    load_sem,
    own_sem,
    state_sem,
    y_send,
    y_recv,
    z_send,
    z_recv,
    late_recv,
    x_send,
    x_recv,
    *buffers,
):
    replicas, experts, tensors, chunks, sorts, late, blocks, pairs, rows = sizes
    widths = chunks + sorts + [late]
    plain = len(chunks)
    count = len(widths) - 1
    raw = buffers[:2]
    arrived = buffers[2 : count + 2]
    outgoing = buffers[count + 2 : 2 * count + 2]
    incoming = buffers[2 * count + 2 : 3 * count + 2]
    staged = buffers[3 * count + 2 : -3]
    late_out, late_in, late_arrived = buffers[-3:]
    my_replica = lax.axis_index("replica")
    my_expert = lax.axis_index("expert")
    my_tensor = lax.axis_index("tensor")
    columns = sum(widths)
    head = sum(sorts)
    edge = head + chunks[0]
    starts = [head + sum(widths[:c]) for c in range(plain)]
    starts += [sum(sorts[:c]) for c in range(count - plain)] + [columns - late]
    groups = [(0, 2), (2, 4), (4, experts)]

    halves = [(0, 2 * pairs), (2 * pairs, blocks)]

    def load(n, d):
        replica = lax.rem(my_replica + d, replicas)
        part = pl.ds(0, edge) if n == 0 else pl.ds(edge, columns - edge)
        return pltpu.make_async_copy(
            delta.at[:, part, replica],
            raw[n].at[d - 1],
            load_sem.at[n, d - 1],
        )

    def arrival(c, h):
        return c + h + max(c - plain, 0)

    def y_copy(c, h, d):
        low, high = halves[h]
        if c == count:
            source, goal = late_in.at[:, d], late_arrived.at[d - 1]
        elif c < plain:
            part = pl.ds(starts[c] - edge if c else head, widths[c])
            source, goal = raw[min(c, 1)].at[d - 1, :, part], arrived[c].at[d - 1]
        else:
            part = (d - 1, pl.ds(low, high - low))
            source, goal = staged[c - plain].at[part], arrived[c].at[part]
        return pltpu.make_async_remote_copy(
            src_ref=source,
            dst_ref=goal,
            send_sem=y_send,
            recv_sem=y_recv.at[arrival(c, h)],
            device_id={"replica": lax.rem(my_replica + d, replicas)},
            device_id_type=MESH,
        )

    def z_copy(c, d):
        part = pl.ds(d * pairs, pairs)
        return pltpu.make_async_remote_copy(
            src_ref=late_out.at[d] if c == count else outgoing[c].at[part],
            dst_ref=late_in.at[d] if c == count else incoming[c].at[part],
            send_sem=z_send,
            recv_sem=late_recv if c == count else z_recv.at[c, group_of(d)],
            device_id={"expert": target(my_expert, d, experts)},
            device_id_type=MESH,
        )

    def sorted_copy(c, e):
        d = between(my_expert, e, experts)
        return pltpu.make_async_remote_copy(
            src_ref=outgoing[c].at[pl.ds(e * pairs, pairs)],
            dst_ref=incoming[c].at[pl.ds(d * pairs, pairs)],
            send_sem=z_send,
            recv_sem=z_recv.at[c, jnp.minimum(lax.div(d, 2), 2)],
            device_id={"expert": e},
            device_id_type=MESH,
        )

    def group_of(d):
        return [g for g, (low, high) in enumerate(groups) if low <= d < high][0]

    def x_copy(c, low, high, d):
        part = (pl.ds(low * pairs, (high - low) * pairs), pl.ds(starts[c], widths[c]))
        return pltpu.make_async_remote_copy(
            src_ref=params_held.at[part],
            dst_ref=params_arrived.at[(d - 1,) + part],
            send_sem=x_send,
            recv_sem=x_recv,
            device_id={"tensor": lax.rem(my_tensor + d, tensors)},
            device_id_type=MESH,
        )

    def all_of(ref, sem):
        return pltpu.make_async_copy(ref, ref, sem)

    barrier = pltpu.get_barrier_semaphore()
    axes = (("expert", my_expert, experts), ("replica", my_replica, replicas), ("tensor", my_tensor, tensors))
    for axis, mine, size in axes:
        for d in reversed(range(1, size)):
            pl.semaphore_signal(
                barrier, inc=1, device_id={axis: lax.rem(mine + d, size)}, device_id_type=MESH
            )
    index_copies = [
        pltpu.make_async_copy(block_map_far, block_map, index_sem.at[0]),
        pltpu.make_async_copy(step_offsets_far, step_offsets, index_sem.at[1]),
    ]
    for copy in index_copies:
        copy.start()
    for n in range(2):
        for d in range(1, replicas):
            load(n, d).start()
    own_load = pltpu.make_async_copy(delta.at[:, :, my_replica], own, own_sem)
    own_load.start()
    for i, source in enumerate((master_params, first_moment, second_moment)):
        pltpu.make_async_copy(source, state.at[i], state_sem).start()

    def digits(key, k):
        return jnp.maximum(lax.rem(lax.div(key, jnp.int32(blocks ** (pairs - 1 - k))), jnp.int32(blocks)), 0)

    def note_order():
        owners = [lax.div(block_map[my_expert * blocks + j], jnp.int32(blocks)) for j in range(blocks)]
        for d in range(experts):
            wanted = target(my_expert, d, experts)
            key = jnp.int32(0)
            for j in range(blocks):
                key = jnp.where(owners[j] == wanted, key * blocks + j, key)
            for k in range(pairs):
                order[d * pairs + k] = digits(key, k)

    def note_slots(d, carry):
        low = origin(my_expert, d, experts) * blocks
        key = jnp.int32(0)
        for j in range(blocks):
            slot = block_map[low + j] - my_expert * blocks
            owned = jnp.where(slot >= 0, slot, blocks) < blocks
            key = jnp.where(owned, key * blocks + slot, key)
        for k in range(pairs):
            slots[d * pairs + k] = digits(key, k)
        return carry

    def note_places(s, carry):
        place = jnp.int32(0)
        for q in range(blocks):
            place = jnp.where(slots[q] == s, q, place)
        places[s] = place
        return carry

    for copy in index_copies:
        copy.wait()
    note_order()
    pl.semaphore_wait(barrier, replicas + experts + tensors - 3)
    def block_of(j):
        return order[between(my_expert, j // pairs, experts) * pairs + j % pairs]

    def gather(c, h):
        dense = widths[c] * rows
        far = raw[0].reshape(replicas - 1, blocks, edge * rows, LANES)
        goal = staged[c - plain].reshape(replicas - 1, blocks, dense, LANES)
        for j in range(*halves[h]):
            for r in range(1, replicas):
                goal[r - 1, j] = far[r - 1, block_of(j), pl.ds(starts[c] * rows, dense)]

    stream = [(c, 0) for c in range(plain, count)] + [(c, 0) for c in range(plain)]
    stream += [(c, 1) for c in range(plain, count)]

    def send(part):
        for c, h in part:
            if c >= plain:
                gather(c, h)
            for d in range(1, replicas):
                y_copy(c, h, d).start()

    for d in range(1, replicas):
        load(0, d).wait()
    first = count - plain + 1
    send(stream[:first])
    for d in range(1, replicas):
        load(1, d).wait()
    send(stream[first:AHEAD])

    own_load.wait()
    late_dense = late * rows
    for d in range(experts):
        held = (late_in if d == 0 else late_out).reshape(experts, replicas, pairs, late_dense, LANES)
        own_flat = own.reshape(blocks, columns * rows, LANES)
        rest = raw[1].reshape(replicas - 1, blocks, (columns - edge) * rows, LANES)
        for k in range(pairs):
            block = order[d * pairs + k]
            held[d, 0, k] = own_flat[block, pl.ds(starts[count] * rows, late_dense)]
            for r in range(1, replicas):
                held[d, r, k] = rest[r - 1, block, pl.ds((starts[count] - edge) * rows, late_dense)]
    for d in reversed(range(1, experts)):
        z_copy(count, d).start()
    send(stream[AHEAD:])

    lax.fori_loop(0, experts, note_slots, 0)
    lax.fori_loop(0, blocks, note_places, 0)

    shares = [
        1.0 / jnp.full((8, LANES), 1 + step_offsets[lax.rem(my_replica + replicas - d, replicas)], jnp.int32).astype(jnp.float32)
        for d in range(replicas)
    ]
    total = functools.reduce(lambda a, b: a + b, shares)
    weights = [(share / total)[:1] for share in shares]

    fix_one = 1.0 - beta_one**outer_round
    fix_two = 1.0 - beta_two**outer_round

    def add_up(c, h):
        low, high = halves[h] if c >= plain else (0, blocks)
        got = arrived[c].at[:, pl.ds(low, high - low)]
        all_of(got, y_recv.at[arrival(c, h)]).wait()
        dense = widths[c] * rows
        part = pl.ds(starts[c] * rows, dense)
        own_flat = own.reshape(blocks, columns * rows, LANES)
        others = arrived[c].reshape(replicas - 1, blocks, dense, LANES)
        out = outgoing[c].reshape(blocks, dense, LANES)
        for q in range(low, high):
            block = block_of(q) if c >= plain else order[q]
            value = own_flat[block, part].astype(jnp.float32) * weights[0]
            for d in range(1, replicas):
                value = value + others[d - 1, q if c >= plain else block].astype(jnp.float32) * weights[d]
            out[q] = value.astype(jnp.bfloat16)

    def adam(c, q, gradient):
        part = pl.ds(starts[c] * rows, widths[c] * rows)
        slot = slots[q]
        one = beta_one * state[1, slot, part] + (1.0 - beta_one) * gradient
        two = beta_two * state[2, slot, part] + (1.0 - beta_two) * gradient * gradient
        first_held[q, part] = one
        second_held[q, part] = two
        update = (outer_rate / fix_one) * one / (jnp.sqrt(two * (1.0 / fix_two)) + epsilon)
        held = params_held.reshape(blocks, columns * rows, LANES)
        held[q, part] = (state[0, slot, part] - update).astype(jnp.bfloat16)

    def finish(c, g):
        low, high = groups[g]
        got = (max(low, 1) * pairs, high * pairs)
        all_of(incoming[c].at[pl.ds(got[0], got[1] - got[0])], z_recv.at[c, g]).wait()
        dense = widths[c] * rows
        for q in range(low * pairs, high * pairs):
            terms = (outgoing[c] if q < pairs else incoming[c]).reshape(blocks, dense, LANES)
            place = my_expert * pairs + q if q < pairs and c >= plain else q
            adam(c, q, terms[place].astype(jnp.float32))
        for d in range(1, tensors):
            x_copy(c, low, high, d).start()

    def finish_late():
        all_of(late_arrived, y_recv.at[arrival(count, 0)]).wait()
        mine = late_in.reshape(experts, replicas, pairs, late_dense, LANES)
        others = late_arrived.reshape(replicas - 1, experts, pairs, late_dense, LANES)
        for q in range(blocks):
            e, k = divmod(q, pairs)
            value = mine[e, 0, k].astype(jnp.float32) * weights[0]
            for d in range(1, replicas):
                value = value + others[d - 1, e, k].astype(jnp.float32) * weights[d]
            adam(count, q, value)
        for d in range(1, tensors):
            x_copy(count, 0, experts, d).start()

    def settle(c):
        part = pl.ds(starts[c] * rows, widths[c] * rows)
        goal = pl.ds(pl.multiple_of((my_tensor * columns + starts[c]) * rows, 8), widths[c] * rows)
        flat = params.reshape(blocks, tensors * columns * rows, LANES)
        held = params_held.reshape(blocks, columns * rows, LANES)
        for s in range(blocks):
            place = places[s]
            new_first[s, part] = first_held[place, part]
            new_second[s, part] = second_held[place, part]
            flat[s, goal] = held[place, part]

    def add_and_send(c, h):
        add_up(c, h)
        if c < plain:
            for d in reversed(range(1, experts)):
                z_copy(c, d).start()
            return
        for e in range(halves[h][0] // pairs, halves[h][1] // pairs):
            pl.when(my_expert != e)(sorted_copy(c, e).start)

    def turn():
        all_of(late_in.at[pl.ds(1, experts - 1)], late_recv).wait()
        for d in range(1, replicas):
            y_copy(count, 0, d).start()

    def ready(c, h, g):
        def act():
            finish(c, g)
            if g == 2:
                settle(c)

        if c < plain:
            act()
        else:
            pl.when(my_expert < 2 if h == 0 else my_expert >= 2)(act)

    def whole_late():
        finish_late()
        settle(count)

    steps = [(TURN, 0, turn)]
    landed = 0
    for c, h in stream:
        landed += widths[c] * (halves[h][1] - halves[h][0]) // blocks if c >= plain else widths[c]
        steps.append((landed, 1, functools.partial(add_and_send, c, h)))
        for g in range(3):
            steps.append((landed + LAGS[g], 3 + g, functools.partial(ready, c, h, g)))
    steps.append((landed + late, 2, whole_late))
    all_of(state, state_sem).wait()
    for _, _, step in sorted(steps, key=lambda entry: entry[:2]):
        step()

    for c in range(count):
        all_of(arrived[c], y_send).wait()
        all_of(incoming[c].at[pl.ds(0, (experts - 1) * pairs)], z_send).wait()
    all_of(late_arrived, y_send).wait()
    all_of(late_in.at[pl.ds(1, experts - 1)], z_send).wait()
    all_of(params_arrived, x_send).wait()
    all_of(params_arrived, x_recv).wait()
    flat = params.reshape(blocks, tensors * columns * rows, LANES)
    others = params_arrived.reshape(tensors - 1, blocks, columns * rows, LANES)
    for d in range(1, tensors):
        sender = lax.rem(my_tensor + tensors - d, tensors)
        goal = pl.ds(pl.multiple_of(sender * columns * rows, 8), columns * rows)
        for s in range(blocks):
            flat[s, goal] = others[d - 1, places[s]]


def write_out(*refs):
    half = (len(refs) - 1) // 2
    sems = refs[-1]
    copies = [
        pltpu.make_async_copy(refs[i], refs[half + i], sems.at[i])
        for i in range(half)
    ]
    for copy in copies:
        copy.start()
    for copy in copies:
        copy.wait()


def split(columns):
    middle = columns - LATE - sum(SORTS)
    return [CHUNK] * (middle // CHUNK), list(SORTS), LATE


def body(delta, step_offsets, block_map, master_params, first_moment, second_moment, *, shape):
    replicas, experts, tensors = shape
    blocks, rows_all, width = delta.shape[1:]
    rows = rows_all // replicas
    columns = width // LANES
    pairs = blocks // experts
    chunks, sorts, late = split(columns)
    widths = chunks + sorts
    count = len(widths)
    edge = sum(sorts) + chunks[0]
    terms = delta.reshape(blocks, replicas, rows, columns, LANES).transpose(0, 3, 1, 2, 4)

    def dense(state):
        split = state.reshape(blocks, rows, columns, LANES).transpose(0, 2, 1, 3)
        return split.reshape(blocks, columns * rows, LANES)

    def undense(state):
        split = state.reshape(blocks, columns, rows, LANES).transpose(0, 2, 1, 3)
        return split.reshape(blocks, rows, width)

    state_shape = (blocks, columns * rows, LANES)
    params_shape = (blocks, tensors * columns, rows, LANES)
    anywhere = pl.BlockSpec(memory_space=pltpu.HBM)
    near = pl.BlockSpec(memory_space=pltpu.VMEM)
    dma = pltpu.SemaphoreType.DMA
    sizes = (replicas, experts, tensors, chunks, sorts, late, blocks, pairs, rows)
    piece = (rows, LANES)
    held = pl.pallas_call(
        functools.partial(kernel, sizes),
        out_shape=(
            pltpu.VMEM(params_shape, jnp.bfloat16),
            pltpu.VMEM(state_shape, jnp.float32),
            pltpu.VMEM(state_shape, jnp.float32),
        ),
        in_specs=[anywhere] * 6,
        out_specs=(near,) * 3,
        scratch_shapes=[
            pltpu.VMEM((3,) + state_shape, jnp.float32),
            pltpu.VMEM(state_shape, jnp.float32),
            pltpu.VMEM(state_shape, jnp.float32),
            pltpu.VMEM((blocks, columns) + piece, jnp.bfloat16),
            pltpu.VMEM((blocks, columns) + piece, jnp.bfloat16),
            pltpu.VMEM((tensors - 1, blocks, columns) + piece, jnp.bfloat16),
            pltpu.SMEM(block_map.shape, jnp.int32),
            pltpu.SMEM(step_offsets.shape, jnp.int32),
            pltpu.SMEM((blocks,), jnp.int32),
            pltpu.SMEM((blocks,), jnp.int32),
            pltpu.SMEM((blocks,), jnp.int32),
            dma((2,)),
            dma((2, replicas - 1)),
            dma,
            dma,
            dma,
            dma((count + len(sorts) + 1,)),
            dma,
            dma((count, 3)),
            dma,
            dma,
            dma,
        ]
        + [pltpu.VMEM((replicas - 1, blocks, c) + piece, jnp.bfloat16) for c in (edge, columns - edge)]
        + [pltpu.VMEM((replicas - 1, blocks, c) + piece, jnp.bfloat16) for c in widths]
        + [pltpu.VMEM((blocks, c) + piece, jnp.bfloat16) for c in widths] * 2
        + [pltpu.VMEM((replicas - 1, blocks, c) + piece, jnp.bfloat16) for c in sorts]
        + [pltpu.VMEM((experts, replicas, pairs, late) + piece, jnp.bfloat16)] * 2
        + [pltpu.VMEM((replicas - 1, experts, pairs, late) + piece, jnp.bfloat16)],
        compiler_params=pltpu.CompilerParams(collective_id=0, has_side_effects=True),
    )(block_map, step_offsets, terms, dense(master_params), dense(first_moment), dense(second_moment))
    new_params, new_first, new_second = pl.pallas_call(
        write_out,
        out_shape=(
            jax.ShapeDtypeStruct(params_shape, jnp.bfloat16),
            jax.ShapeDtypeStruct(state_shape, jnp.float32),
            jax.ShapeDtypeStruct(state_shape, jnp.float32),
        ),
        in_specs=[near] * 3,
        out_specs=(anywhere,) * 3,
        scratch_shapes=[dma((3,))],
        compiler_params=pltpu.CompilerParams(vmem_limit_bytes=1024 * 1024),
    )(*held)
    full = new_params.transpose(0, 2, 1, 3).reshape(blocks, rows, tensors * width)
    return (full, undense(new_first), undense(new_second))


def solution(mesh):
    in_specs = (
        P("replica", "expert", None, "tensor"),
        P(),
        P(),
        P("expert", "replica", "tensor"),
        P("expert", "replica", "tensor"),
        P("expert", "replica", "tensor"),
    )
    out_specs = (
        P("expert", "replica", None),
        P("expert", "replica", "tensor"),
        P("expert", "replica", "tensor"),
    )
    shape = tuple(mesh.shape[axis] for axis in ("replica", "expert", "tensor"))
    step = functools.partial(body, shape=shape)
    return jax.shard_map(step, mesh=mesh, in_specs=in_specs, out_specs=out_specs, check_vma=False)
```

```python
import functools

import jax
import jax.numpy as jnp
from jax import lax
from jax.experimental import pallas as pl
from jax.experimental.pallas import tpu as pltpu
from jax.sharding import PartitionSpec as P

beta_one = 0.9
beta_two = 0.99
outer_rate = 0.7
outer_round = 20
epsilon = 1e-08

LANES = 128
CHUNK = 4
LATE = 8
SORTS = (4, 4, 4)
AHEAD = 7
TURN = 21
LAGS = (8, 16, 24)
MESH = pl.DeviceIdType.MESH


def target(mine, d, size):
    if size & (size - 1):
        return lax.rem(mine + d, size)
    if not isinstance(d, int):
        peer = mine
        bit = 1
        while bit < size:
            both = lax.rem(lax.div(mine, bit), 2) * lax.rem(lax.div(d, bit), 2)
            peer = peer + bit * (lax.rem(lax.div(d, bit), 2) - 2 * both)
            bit *= 2
        return peer
    peer = mine
    bit = 1
    while bit < size:
        if d & bit:
            peer = peer + bit * (1 - 2 * lax.rem(lax.div(mine, bit), 2))
        bit *= 2
    return peer


def between(mine, peer, size):
    if size & (size - 1):
        return lax.rem(peer + size - mine, size)
    return target(mine, peer, size)


def origin(mine, d, size):
    if size & (size - 1):
        return lax.rem(mine + size - d, size)
    return target(mine, d, size)


def kernel(
    sizes,
    block_map_far,
    step_offsets_far,
    delta,
    master_params,
    first_moment,
    second_moment,
    params,
    new_first,
    new_second,
    state,
    first_held,
    second_held,
    own,
    params_held,
    params_arrived,
    block_map,
    step_offsets,
    order,
    slots,
    places,
    index_sem,
    load_sem,
    own_sem,
    state_sem,
    y_send,
    y_recv,
    z_send,
    z_recv,
    late_recv,
    x_send,
    x_recv,
    *buffers,
):
    replicas, experts, tensors, chunks, sorts, late, blocks, pairs, rows = sizes
    widths = chunks + sorts + [late]
    plain = len(chunks)
    count = len(widths) - 1
    raw = buffers[:2]
    arrived = buffers[2 : count + 2]
    outgoing = buffers[count + 2 : 2 * count + 2]
    incoming = buffers[2 * count + 2 : 3 * count + 2]
    staged = buffers[3 * count + 2 : -3]
    late_out, late_in, late_arrived = buffers[-3:]
    my_replica = lax.axis_index("replica")
    my_expert = lax.axis_index("expert")
    my_tensor = lax.axis_index("tensor")
    columns = sum(widths)
    head = sum(sorts)
    edge = head + chunks[0]
    starts = [head + sum(widths[:c]) for c in range(plain)]
    starts += [sum(sorts[:c]) for c in range(count - plain)] + [columns - late]
    groups = [(0, 2), (2, 4), (4, experts)]

    halves = [(0, 2 * pairs), (2 * pairs, blocks)]

    def load(n, d):
        replica = lax.rem(my_replica + d, replicas)
        part = pl.ds(0, edge) if n == 0 else pl.ds(edge, columns - edge)
        return pltpu.make_async_copy(
            delta.at[:, part, replica],
            raw[n].at[d - 1],
            load_sem.at[n, d - 1],
        )

    def arrival(c, h):
        return c + h + max(c - plain, 0)

    def y_copy(c, h, d):
        low, high = halves[h]
        if c == count:
            source, goal = late_in.at[:, d], late_arrived.at[d - 1]
        elif c < plain:
            part = pl.ds(starts[c] - edge if c else head, widths[c])
            source, goal = raw[min(c, 1)].at[d - 1, :, part], arrived[c].at[d - 1]
        else:
            part = (d - 1, pl.ds(low, high - low))
            source, goal = staged[c - plain].at[part], arrived[c].at[part]
        return pltpu.make_async_remote_copy(
            src_ref=source,
            dst_ref=goal,
            send_sem=y_send,
            recv_sem=y_recv.at[arrival(c, h)],
            device_id={"replica": lax.rem(my_replica + d, replicas)},
            device_id_type=MESH,
        )

    def z_copy(c, d):
        part = pl.ds(d * pairs, pairs)
        return pltpu.make_async_remote_copy(
            src_ref=late_out.at[d] if c == count else outgoing[c].at[part],
            dst_ref=late_in.at[d] if c == count else incoming[c].at[part],
            send_sem=z_send,
            recv_sem=late_recv if c == count else z_recv.at[c, group_of(d)],
            device_id={"expert": target(my_expert, d, experts)},
            device_id_type=MESH,
        )

    def sorted_copy(c, e):
        d = between(my_expert, e, experts)
        return pltpu.make_async_remote_copy(
            src_ref=outgoing[c].at[pl.ds(e * pairs, pairs)],
            dst_ref=incoming[c].at[pl.ds(d * pairs, pairs)],
            send_sem=z_send,
            recv_sem=z_recv.at[c, jnp.minimum(lax.div(d, 2), 2)],
            device_id={"expert": e},
            device_id_type=MESH,
        )

    def group_of(d):
        return [g for g, (low, high) in enumerate(groups) if low <= d < high][0]

    def x_copy(c, low, high, d):
        part = (pl.ds(low * pairs, (high - low) * pairs), pl.ds(starts[c], widths[c]))
        return pltpu.make_async_remote_copy(
            src_ref=params_held.at[part],
            dst_ref=params_arrived.at[(d - 1,) + part],
            send_sem=x_send,
            recv_sem=x_recv,
            device_id={"tensor": lax.rem(my_tensor + d, tensors)},
            device_id_type=MESH,
        )

    def all_of(ref, sem):
        return pltpu.make_async_copy(ref, ref, sem)

    barrier = pltpu.get_barrier_semaphore()
    axes = (("expert", my_expert, experts), ("replica", my_replica, replicas), ("tensor", my_tensor, tensors))
    for axis, mine, size in axes:
        for d in reversed(range(1, size)):
            pl.semaphore_signal(
                barrier, inc=1, device_id={axis: lax.rem(mine + d, size)}, device_id_type=MESH
            )
    index_copies = [
        pltpu.make_async_copy(block_map_far, block_map, index_sem.at[0]),
        pltpu.make_async_copy(step_offsets_far, step_offsets, index_sem.at[1]),
    ]
    for copy in index_copies:
        copy.start()
    for n in range(2):
        for d in range(1, replicas):
            load(n, d).start()
    own_load = pltpu.make_async_copy(delta.at[:, :, my_replica], own, own_sem)
    own_load.start()
    for i, source in enumerate((master_params, first_moment, second_moment)):
        pltpu.make_async_copy(source, state.at[i], state_sem).start()

    def digits(key, k):
        return jnp.maximum(lax.rem(lax.div(key, jnp.int32(blocks ** (pairs - 1 - k))), jnp.int32(blocks)), 0)

    def note_order():
        owners = [lax.div(block_map[my_expert * blocks + j], jnp.int32(blocks)) for j in range(blocks)]
        for d in range(experts):
            wanted = target(my_expert, d, experts)
            key = jnp.int32(0)
            for j in range(blocks):
                key = jnp.where(owners[j] == wanted, key * blocks + j, key)
            for k in range(pairs):
                order[d * pairs + k] = digits(key, k)

    def note_slots(d, carry):
        low = origin(my_expert, d, experts) * blocks
        key = jnp.int32(0)
        for j in range(blocks):
            slot = block_map[low + j] - my_expert * blocks
            owned = jnp.where(slot >= 0, slot, blocks) < blocks
            key = jnp.where(owned, key * blocks + slot, key)
        for k in range(pairs):
            slots[d * pairs + k] = digits(key, k)
        return carry

    def note_places(s, carry):
        place = jnp.int32(0)
        for q in range(blocks):
            place = jnp.where(slots[q] == s, q, place)
        places[s] = place
        return carry

    for copy in index_copies:
        copy.wait()
    note_order()
    pl.semaphore_wait(barrier, replicas + experts + tensors - 3)
    def block_of(j):
        return order[between(my_expert, j // pairs, experts) * pairs + j % pairs]

    def gather(c, h):
        dense = widths[c] * rows
        far = raw[0].reshape(replicas - 1, blocks, edge * rows, LANES)
        goal = staged[c - plain].reshape(replicas - 1, blocks, dense, LANES)
        for j in range(*halves[h]):
            for r in range(1, replicas):
                goal[r - 1, j] = far[r - 1, block_of(j), pl.ds(starts[c] * rows, dense)]

    stream = [(c, 0) for c in range(plain, count)] + [(c, 0) for c in range(plain)]
    stream += [(c, 1) for c in range(plain, count)]

    def send(part):
        for c, h in part:
            if c >= plain:
                gather(c, h)
            for d in range(1, replicas):
                y_copy(c, h, d).start()

    for d in range(1, replicas):
        load(0, d).wait()
    first = count - plain + 1
    send(stream[:first])
    for d in range(1, replicas):
        load(1, d).wait()
    send(stream[first:AHEAD])

    own_load.wait()
    late_dense = late * rows
    for d in range(experts):
        held = (late_in if d == 0 else late_out).reshape(experts, replicas, pairs, late_dense, LANES)
        own_flat = own.reshape(blocks, columns * rows, LANES)
        rest = raw[1].reshape(replicas - 1, blocks, (columns - edge) * rows, LANES)
        for k in range(pairs):
            block = order[d * pairs + k]
            held[d, 0, k] = own_flat[block, pl.ds(starts[count] * rows, late_dense)]
            for r in range(1, replicas):
                held[d, r, k] = rest[r - 1, block, pl.ds((starts[count] - edge) * rows, late_dense)]
    for d in reversed(range(1, experts)):
        z_copy(count, d).start()
    send(stream[AHEAD:])

    lax.fori_loop(0, experts, note_slots, 0)
    lax.fori_loop(0, blocks, note_places, 0)

    shares = [
        1.0 / jnp.full((8, LANES), 1 + step_offsets[lax.rem(my_replica + replicas - d, replicas)], jnp.int32).astype(jnp.float32)
        for d in range(replicas)
    ]
    total = functools.reduce(lambda a, b: a + b, shares)
    weights = [(share / total)[:1] for share in shares]

    fix_one = 1.0 - beta_one**outer_round
    fix_two = 1.0 - beta_two**outer_round

    def add_up(c, h):
        low, high = halves[h] if c >= plain else (0, blocks)
        got = arrived[c].at[:, pl.ds(low, high - low)]
        all_of(got, y_recv.at[arrival(c, h)]).wait()
        dense = widths[c] * rows
        part = pl.ds(starts[c] * rows, dense)
        own_flat = own.reshape(blocks, columns * rows, LANES)
        others = arrived[c].reshape(replicas - 1, blocks, dense, LANES)
        out = outgoing[c].reshape(blocks, dense, LANES)
        for q in range(low, high):
            block = block_of(q) if c >= plain else order[q]
            value = own_flat[block, part].astype(jnp.float32) * weights[0]
            for d in range(1, replicas):
                value = value + others[d - 1, q if c >= plain else block].astype(jnp.float32) * weights[d]
            out[q] = value.astype(jnp.bfloat16)

    def adam(c, q, gradient):
        part = pl.ds(starts[c] * rows, widths[c] * rows)
        slot = slots[q]
        one = beta_one * state[1, slot, part] + (1.0 - beta_one) * gradient
        two = beta_two * state[2, slot, part] + (1.0 - beta_two) * gradient * gradient
        first_held[q, part] = one
        second_held[q, part] = two
        update = (outer_rate / fix_one) * one / (jnp.sqrt(two * (1.0 / fix_two)) + epsilon)
        held = params_held.reshape(blocks, columns * rows, LANES)
        held[q, part] = (state[0, slot, part] - update).astype(jnp.bfloat16)

    def finish(c, g):
        low, high = groups[g]
        got = (max(low, 1) * pairs, high * pairs)
        all_of(incoming[c].at[pl.ds(got[0], got[1] - got[0])], z_recv.at[c, g]).wait()
        dense = widths[c] * rows
        for q in range(low * pairs, high * pairs):
            terms = (outgoing[c] if q < pairs else incoming[c]).reshape(blocks, dense, LANES)
            place = my_expert * pairs + q if q < pairs and c >= plain else q
            adam(c, q, terms[place].astype(jnp.float32))
        for d in range(1, tensors):
            x_copy(c, low, high, d).start()

    def finish_late():
        all_of(late_arrived, y_recv.at[arrival(count, 0)]).wait()
        mine = late_in.reshape(experts, replicas, pairs, late_dense, LANES)
        others = late_arrived.reshape(replicas - 1, experts, pairs, late_dense, LANES)
        for q in range(blocks):
            e, k = divmod(q, pairs)
            value = mine[e, 0, k].astype(jnp.float32) * weights[0]
            for d in range(1, replicas):
                value = value + others[d - 1, e, k].astype(jnp.float32) * weights[d]
            adam(count, q, value)
        for d in range(1, tensors):
            x_copy(count, 0, experts, d).start()

    def settle(c):
        part = pl.ds(starts[c] * rows, widths[c] * rows)
        goal = pl.ds(pl.multiple_of((my_tensor * columns + starts[c]) * rows, 8), widths[c] * rows)
        flat = params.reshape(blocks, tensors * columns * rows, LANES)
        held = params_held.reshape(blocks, columns * rows, LANES)
        for s in range(blocks):
            place = places[s]
            new_first[s, part] = first_held[place, part]
            new_second[s, part] = second_held[place, part]
            flat[s, goal] = held[place, part]

    def add_and_send(c, h):
        add_up(c, h)
        if c < plain:
            for d in reversed(range(1, experts)):
                z_copy(c, d).start()
            return
        for e in range(halves[h][0] // pairs, halves[h][1] // pairs):
            pl.when(my_expert != e)(sorted_copy(c, e).start)

    def turn():
        all_of(late_in.at[pl.ds(1, experts - 1)], late_recv).wait()
        for d in range(1, replicas):
            y_copy(count, 0, d).start()

    def ready(c, h, g):
        def act():
            finish(c, g)
            if g == 2:
                settle(c)

        if c < plain:
            act()
        else:
            pl.when(my_expert < 2 if h == 0 else my_expert >= 2)(act)

    def whole_late():
        finish_late()
        settle(count)

    steps = [(TURN, 0, turn)]
    landed = 0
    for c, h in stream:
        landed += widths[c] * (halves[h][1] - halves[h][0]) // blocks if c >= plain else widths[c]
        steps.append((landed, 1, functools.partial(add_and_send, c, h)))
        for g in range(3):
            steps.append((landed + LAGS[g], 3 + g, functools.partial(ready, c, h, g)))
    steps.append((landed + late, 2, whole_late))
    all_of(state, state_sem).wait()
    for _, _, step in sorted(steps, key=lambda entry: entry[:2]):
        step()

    for c in range(count):
        all_of(arrived[c], y_send).wait()
        all_of(incoming[c].at[pl.ds(0, (experts - 1) * pairs)], z_send).wait()
    all_of(late_arrived, y_send).wait()
    all_of(late_in.at[pl.ds(1, experts - 1)], z_send).wait()
    all_of(params_arrived, x_send).wait()
    all_of(params_arrived, x_recv).wait()
    flat = params.reshape(blocks, tensors * columns * rows, LANES)
    others = params_arrived.reshape(tensors - 1, blocks, columns * rows, LANES)
    for d in range(1, tensors):
        sender = lax.rem(my_tensor + tensors - d, tensors)
        goal = pl.ds(pl.multiple_of(sender * columns * rows, 8), columns * rows)
        for s in range(blocks):
            flat[s, goal] = others[d - 1, places[s]]


def write_out(*refs):
    half = (len(refs) - 1) // 2
    sems = refs[-1]
    copies = [
        pltpu.make_async_copy(refs[i], refs[half + i], sems.at[i])
        for i in range(half)
    ]
    for copy in copies:
        copy.start()
    for copy in copies:
        copy.wait()


def split(columns):
    middle = columns - LATE - sum(SORTS)
    return [CHUNK] * (middle // CHUNK), list(SORTS), LATE


def body(delta, step_offsets, block_map, master_params, first_moment, second_moment, *, shape):
    replicas, experts, tensors = shape
    blocks, rows_all, width = delta.shape[1:]
    rows = rows_all // replicas
    columns = width // LANES
    pairs = blocks // experts
    chunks, sorts, late = split(columns)
    widths = chunks + sorts
    count = len(widths)
    edge = sum(sorts) + chunks[0]
    terms = delta.reshape(blocks, replicas, rows, columns, LANES).transpose(0, 3, 1, 2, 4)

    def dense(state):
        split = state.reshape(blocks, rows, columns, LANES).transpose(0, 2, 1, 3)
        return split.reshape(blocks, columns * rows, LANES)

    def undense(state):
        split = state.reshape(blocks, columns, rows, LANES).transpose(0, 2, 1, 3)
        return split.reshape(blocks, rows, width)

    state_shape = (blocks, columns * rows, LANES)
    params_shape = (blocks, tensors * columns, rows, LANES)
    anywhere = pl.BlockSpec(memory_space=pltpu.HBM)
    near = pl.BlockSpec(memory_space=pltpu.VMEM)
    dma = pltpu.SemaphoreType.DMA
    sizes = (replicas, experts, tensors, chunks, sorts, late, blocks, pairs, rows)
    piece = (rows, LANES)
    held = pl.pallas_call(
        functools.partial(kernel, sizes),
        out_shape=(
            pltpu.VMEM(params_shape, jnp.bfloat16),
            pltpu.VMEM(state_shape, jnp.float32),
            pltpu.VMEM(state_shape, jnp.float32),
        ),
        in_specs=[anywhere] * 6,
        out_specs=(near,) * 3,
        scratch_shapes=[
            pltpu.VMEM((3,) + state_shape, jnp.float32),
            pltpu.VMEM(state_shape, jnp.float32),
            pltpu.VMEM(state_shape, jnp.float32),
            pltpu.VMEM((blocks, columns) + piece, jnp.bfloat16),
            pltpu.VMEM((blocks, columns) + piece, jnp.bfloat16),
            pltpu.VMEM((tensors - 1, blocks, columns) + piece, jnp.bfloat16),
            pltpu.SMEM(block_map.shape, jnp.int32),
            pltpu.SMEM(step_offsets.shape, jnp.int32),
            pltpu.SMEM((blocks,), jnp.int32),
            pltpu.SMEM((blocks,), jnp.int32),
            pltpu.SMEM((blocks,), jnp.int32),
            dma((2,)),
            dma((2, replicas - 1)),
            dma,
            dma,
            dma,
            dma((count + len(sorts) + 1,)),
            dma,
            dma((count, 3)),
            dma,
            dma,
            dma,
        ]
        + [pltpu.VMEM((replicas - 1, blocks, c) + piece, jnp.bfloat16) for c in (edge, columns - edge)]
        + [pltpu.VMEM((replicas - 1, blocks, c) + piece, jnp.bfloat16) for c in widths]
        + [pltpu.VMEM((blocks, c) + piece, jnp.bfloat16) for c in widths] * 2
        + [pltpu.VMEM((replicas - 1, blocks, c) + piece, jnp.bfloat16) for c in sorts]
        + [pltpu.VMEM((experts, replicas, pairs, late) + piece, jnp.bfloat16)] * 2
        + [pltpu.VMEM((replicas - 1, experts, pairs, late) + piece, jnp.bfloat16)],
        compiler_params=pltpu.CompilerParams(collective_id=0, has_side_effects=True),
    )(block_map, step_offsets, terms, dense(master_params), dense(first_moment), dense(second_moment))
    new_params, new_first, new_second = pl.pallas_call(
        write_out,
        out_shape=(
            jax.ShapeDtypeStruct(params_shape, jnp.bfloat16),
            jax.ShapeDtypeStruct(state_shape, jnp.float32),
            jax.ShapeDtypeStruct(state_shape, jnp.float32),
        ),
        in_specs=[near] * 3,
        out_specs=(anywhere,) * 3,
        scratch_shapes=[dma((3,))],
        compiler_params=pltpu.CompilerParams(vmem_limit_bytes=1024 * 1024),
    )(*held)
    full = new_params.transpose(0, 2, 1, 3).reshape(blocks, rows, tensors * width)
    return (full, undense(new_first), undense(new_second))


def solution(mesh):
    in_specs = (
        P("replica", "expert", None, "tensor"),
        P(),
        P(),
        P("expert", "replica", "tensor"),
        P("expert", "replica", "tensor"),
        P("expert", "replica", "tensor"),
    )
    out_specs = (
        P("expert", "replica", None),
        P("expert", "replica", "tensor"),
        P("expert", "replica", "tensor"),
    )
    shape = tuple(mesh.shape[axis] for axis in ("replica", "expert", "tensor"))
    step = functools.partial(body, shape=shape)
    return jax.shard_map(step, mesh=mesh, in_specs=in_specs, out_specs=out_specs, check_vma=False)
```

```python
import functools

import jax
import jax.numpy as jnp
from jax import lax
from jax.experimental import pallas as pl
from jax.experimental.pallas import tpu as pltpu
from jax.sharding import PartitionSpec as P

beta_one = 0.9
beta_two = 0.99
outer_rate = 0.7
outer_round = 20
epsilon = 1e-08

LANES = 128
CHUNK = 4
LATE = 8
SORTS = (4, 4, 4)
AHEAD = 7
TURN = 21
LAGS = (8, 16, 23)
MESH = pl.DeviceIdType.MESH


def target(mine, d, size):
    if size & (size - 1):
        return lax.rem(mine + d, size)
    if not isinstance(d, int):
        peer = mine
        bit = 1
        while bit < size:
            both = lax.rem(lax.div(mine, bit), 2) * lax.rem(lax.div(d, bit), 2)
            peer = peer + bit * (lax.rem(lax.div(d, bit), 2) - 2 * both)
            bit *= 2
        return peer
    peer = mine
    bit = 1
    while bit < size:
        if d & bit:
            peer = peer + bit * (1 - 2 * lax.rem(lax.div(mine, bit), 2))
        bit *= 2
    return peer


def between(mine, peer, size):
    if size & (size - 1):
        return lax.rem(peer + size - mine, size)
    return target(mine, peer, size)


def origin(mine, d, size):
    if size & (size - 1):
        return lax.rem(mine + size - d, size)
    return target(mine, d, size)


def kernel(
    sizes,
    block_map_far,
    step_offsets_far,
    delta,
    master_params,
    first_moment,
    second_moment,
    params,
    new_first,
    new_second,
    state,
    first_held,
    second_held,
    own,
    params_held,
    params_arrived,
    block_map,
    step_offsets,
    order,
    slots,
    places,
    index_sem,
    load_sem,
    own_sem,
    state_sem,
    y_send,
    y_recv,
    z_send,
    z_recv,
    late_recv,
    x_send,
    x_recv,
    *buffers,
):
    replicas, experts, tensors, chunks, sorts, late, blocks, pairs, rows = sizes
    widths = chunks + sorts + [late]
    plain = len(chunks)
    count = len(widths) - 1
    raw = buffers[:2]
    arrived = buffers[2 : count + 2]
    outgoing = buffers[count + 2 : 2 * count + 2]
    incoming = buffers[2 * count + 2 : 3 * count + 2]
    staged = buffers[3 * count + 2 : -3]
    late_out, late_in, late_arrived = buffers[-3:]
    my_replica = lax.axis_index("replica")
    my_expert = lax.axis_index("expert")
    my_tensor = lax.axis_index("tensor")
    columns = sum(widths)
    head = sum(sorts)
    edge = head + chunks[0]
    starts = [head + sum(widths[:c]) for c in range(plain)]
    starts += [sum(sorts[:c]) for c in range(count - plain)] + [columns - late]
    groups = [(0, 2), (2, 4), (4, experts)]

    halves = [(0, 2 * pairs), (2 * pairs, blocks)]

    def load(n, d):
        replica = lax.rem(my_replica + d, replicas)
        part = pl.ds(0, edge) if n == 0 else pl.ds(edge, columns - edge)
        return pltpu.make_async_copy(
            delta.at[:, part, replica],
            raw[n].at[d - 1],
            load_sem.at[n, d - 1],
        )

    def arrival(c, h):
        return c + h + max(c - plain, 0)

    def y_copy(c, h, d):
        low, high = halves[h]
        if c == count:
            source, goal = late_in.at[:, d], late_arrived.at[d - 1]
        elif c < plain:
            part = pl.ds(starts[c] - edge if c else head, widths[c])
            source, goal = raw[min(c, 1)].at[d - 1, :, part], arrived[c].at[d - 1]
        else:
            part = (d - 1, pl.ds(low, high - low))
            source, goal = staged[c - plain].at[part], arrived[c].at[part]
        return pltpu.make_async_remote_copy(
            src_ref=source,
            dst_ref=goal,
            send_sem=y_send,
            recv_sem=y_recv.at[arrival(c, h)],
            device_id={"replica": lax.rem(my_replica + d, replicas)},
            device_id_type=MESH,
        )

    def z_copy(c, d):
        part = pl.ds(d * pairs, pairs)
        return pltpu.make_async_remote_copy(
            src_ref=late_out.at[d] if c == count else outgoing[c].at[part],
            dst_ref=late_in.at[d] if c == count else incoming[c].at[part],
            send_sem=z_send,
            recv_sem=late_recv if c == count else z_recv.at[c, group_of(d)],
            device_id={"expert": target(my_expert, d, experts)},
            device_id_type=MESH,
        )

    def sorted_copy(c, e):
        d = between(my_expert, e, experts)
        return pltpu.make_async_remote_copy(
            src_ref=outgoing[c].at[pl.ds(e * pairs, pairs)],
            dst_ref=incoming[c].at[pl.ds(d * pairs, pairs)],
            send_sem=z_send,
            recv_sem=z_recv.at[c, jnp.minimum(lax.div(d, 2), 2)],
            device_id={"expert": e},
            device_id_type=MESH,
        )

    def group_of(d):
        return [g for g, (low, high) in enumerate(groups) if low <= d < high][0]

    def x_copy(c, low, high, d):
        part = (pl.ds(low * pairs, (high - low) * pairs), pl.ds(starts[c], widths[c]))
        return pltpu.make_async_remote_copy(
            src_ref=params_held.at[part],
            dst_ref=params_arrived.at[(d - 1,) + part],
            send_sem=x_send,
            recv_sem=x_recv,
            device_id={"tensor": lax.rem(my_tensor + d, tensors)},
            device_id_type=MESH,
        )

    def all_of(ref, sem):
        return pltpu.make_async_copy(ref, ref, sem)

    barrier = pltpu.get_barrier_semaphore()
    axes = (("expert", my_expert, experts), ("replica", my_replica, replicas), ("tensor", my_tensor, tensors))
    for axis, mine, size in axes:
        for d in reversed(range(1, size)):
            pl.semaphore_signal(
                barrier, inc=1, device_id={axis: lax.rem(mine + d, size)}, device_id_type=MESH
            )
    index_copies = [
        pltpu.make_async_copy(block_map_far, block_map, index_sem.at[0]),
        pltpu.make_async_copy(step_offsets_far, step_offsets, index_sem.at[1]),
    ]
    for copy in index_copies:
        copy.start()
    for n in range(2):
        for d in range(1, replicas):
            load(n, d).start()
    own_load = pltpu.make_async_copy(delta.at[:, :, my_replica], own, own_sem)
    own_load.start()
    for i, source in enumerate((master_params, first_moment, second_moment)):
        pltpu.make_async_copy(source, state.at[i], state_sem).start()

    def digits(key, k):
        return jnp.maximum(lax.rem(lax.div(key, jnp.int32(blocks ** (pairs - 1 - k))), jnp.int32(blocks)), 0)

    def note_order():
        owners = [lax.div(block_map[my_expert * blocks + j], jnp.int32(blocks)) for j in range(blocks)]
        for d in range(experts):
            wanted = target(my_expert, d, experts)
            key = jnp.int32(0)
            for j in range(blocks):
                key = jnp.where(owners[j] == wanted, key * blocks + j, key)
            for k in range(pairs):
                order[d * pairs + k] = digits(key, k)

    def note_slots(d, carry):
        low = origin(my_expert, d, experts) * blocks
        key = jnp.int32(0)
        for j in range(blocks):
            slot = block_map[low + j] - my_expert * blocks
            owned = jnp.where(slot >= 0, slot, blocks) < blocks
            key = jnp.where(owned, key * blocks + slot, key)
        for k in range(pairs):
            slots[d * pairs + k] = digits(key, k)
        return carry

    def note_places(s, carry):
        place = jnp.int32(0)
        for q in range(blocks):
            place = jnp.where(slots[q] == s, q, place)
        places[s] = place
        return carry

    for copy in index_copies:
        copy.wait()
    note_order()
    pl.semaphore_wait(barrier, replicas + experts + tensors - 3)
    def block_of(j):
        return order[between(my_expert, j // pairs, experts) * pairs + j % pairs]

    def gather(c, h):
        dense = widths[c] * rows
        far = raw[0].reshape(replicas - 1, blocks, edge * rows, LANES)
        goal = staged[c - plain].reshape(replicas - 1, blocks, dense, LANES)
        for j in range(*halves[h]):
            for r in range(1, replicas):
                goal[r - 1, j] = far[r - 1, block_of(j), pl.ds(starts[c] * rows, dense)]

    stream = [(c, 0) for c in range(plain, count)] + [(c, 0) for c in range(plain)]
    stream += [(c, 1) for c in range(plain, count)]

    def send(part):
        for c, h in part:
            if c >= plain:
                gather(c, h)
            for d in range(1, replicas):
                y_copy(c, h, d).start()

    for d in range(1, replicas):
        load(0, d).wait()
    first = count - plain + 1
    send(stream[:first])
    for d in range(1, replicas):
        load(1, d).wait()
    send(stream[first:AHEAD])

    own_load.wait()
    late_dense = late * rows
    for d in range(experts):
        held = (late_in if d == 0 else late_out).reshape(experts, replicas, pairs, late_dense, LANES)
        own_flat = own.reshape(blocks, columns * rows, LANES)
        rest = raw[1].reshape(replicas - 1, blocks, (columns - edge) * rows, LANES)
        for k in range(pairs):
            block = order[d * pairs + k]
            held[d, 0, k] = own_flat[block, pl.ds(starts[count] * rows, late_dense)]
            for r in range(1, replicas):
                held[d, r, k] = rest[r - 1, block, pl.ds((starts[count] - edge) * rows, late_dense)]
    for d in reversed(range(1, experts)):
        z_copy(count, d).start()
    send(stream[AHEAD:])

    lax.fori_loop(0, experts, note_slots, 0)
    lax.fori_loop(0, blocks, note_places, 0)

    shares = [
        1.0 / jnp.full((8, LANES), 1 + step_offsets[lax.rem(my_replica + replicas - d, replicas)], jnp.int32).astype(jnp.float32)
        for d in range(replicas)
    ]
    total = functools.reduce(lambda a, b: a + b, shares)
    weights = [(share / total)[:1] for share in shares]

    fix_one = 1.0 - beta_one**outer_round
    fix_two = 1.0 - beta_two**outer_round

    def add_up(c, h):
        low, high = halves[h] if c >= plain else (0, blocks)
        got = arrived[c].at[:, pl.ds(low, high - low)]
        all_of(got, y_recv.at[arrival(c, h)]).wait()
        dense = widths[c] * rows
        part = pl.ds(starts[c] * rows, dense)
        own_flat = own.reshape(blocks, columns * rows, LANES)
        others = arrived[c].reshape(replicas - 1, blocks, dense, LANES)
        out = outgoing[c].reshape(blocks, dense, LANES)
        for q in range(low, high):
            block = block_of(q) if c >= plain else order[q]
            value = own_flat[block, part].astype(jnp.float32) * weights[0]
            for d in range(1, replicas):
                value = value + others[d - 1, q if c >= plain else block].astype(jnp.float32) * weights[d]
            out[q] = value.astype(jnp.bfloat16)

    def adam(c, q, gradient):
        part = pl.ds(starts[c] * rows, widths[c] * rows)
        slot = slots[q]
        one = beta_one * state[1, slot, part] + (1.0 - beta_one) * gradient
        two = beta_two * state[2, slot, part] + (1.0 - beta_two) * gradient * gradient
        first_held[q, part] = one
        second_held[q, part] = two
        update = (outer_rate / fix_one) * one / (jnp.sqrt(two * (1.0 / fix_two)) + epsilon)
        held = params_held.reshape(blocks, columns * rows, LANES)
        held[q, part] = (state[0, slot, part] - update).astype(jnp.bfloat16)

    def finish(c, g):
        low, high = groups[g]
        got = (max(low, 1) * pairs, high * pairs)
        all_of(incoming[c].at[pl.ds(got[0], got[1] - got[0])], z_recv.at[c, g]).wait()
        dense = widths[c] * rows
        for q in range(low * pairs, high * pairs):
            terms = (outgoing[c] if q < pairs else incoming[c]).reshape(blocks, dense, LANES)
            place = my_expert * pairs + q if q < pairs and c >= plain else q
            adam(c, q, terms[place].astype(jnp.float32))
        for d in range(1, tensors):
            x_copy(c, low, high, d).start()

    def finish_late():
        all_of(late_arrived, y_recv.at[arrival(count, 0)]).wait()
        mine = late_in.reshape(experts, replicas, pairs, late_dense, LANES)
        others = late_arrived.reshape(replicas - 1, experts, pairs, late_dense, LANES)
        for q in range(blocks):
            e, k = divmod(q, pairs)
            value = mine[e, 0, k].astype(jnp.float32) * weights[0]
            for d in range(1, replicas):
                value = value + others[d - 1, e, k].astype(jnp.float32) * weights[d]
            adam(count, q, value)
        for d in range(1, tensors):
            x_copy(count, 0, experts, d).start()

    def settle(c):
        part = pl.ds(starts[c] * rows, widths[c] * rows)
        goal = pl.ds(pl.multiple_of((my_tensor * columns + starts[c]) * rows, 8), widths[c] * rows)
        flat = params.reshape(blocks, tensors * columns * rows, LANES)
        held = params_held.reshape(blocks, columns * rows, LANES)
        for s in range(blocks):
            place = places[s]
            new_first[s, part] = first_held[place, part]
            new_second[s, part] = second_held[place, part]
            flat[s, goal] = held[place, part]

    def add_and_send(c, h):
        add_up(c, h)
        if c < plain:
            for d in reversed(range(1, experts)):
                z_copy(c, d).start()
            return
        for e in range(halves[h][0] // pairs, halves[h][1] // pairs):
            pl.when(my_expert != e)(sorted_copy(c, e).start)

    def turn():
        all_of(late_in.at[pl.ds(1, experts - 1)], late_recv).wait()
        for d in range(1, replicas):
            y_copy(count, 0, d).start()

    def ready(c, h, g):
        def act():
            finish(c, g)
            if g == 2:
                settle(c)

        if c < plain:
            act()
        else:
            pl.when(my_expert < 2 if h == 0 else my_expert >= 2)(act)

    def whole_late():
        finish_late()
        settle(count)

    steps = [(TURN, 0, turn)]
    landed = 0
    for c, h in stream:
        landed += widths[c] * (halves[h][1] - halves[h][0]) // blocks if c >= plain else widths[c]
        steps.append((landed, 1, functools.partial(add_and_send, c, h)))
        for g in range(3):
            steps.append((landed + LAGS[g], 3 + g, functools.partial(ready, c, h, g)))
    steps.append((landed + late, 2, whole_late))
    all_of(state, state_sem).wait()
    for _, _, step in sorted(steps, key=lambda entry: entry[:2]):
        step()

    for c in range(count):
        all_of(arrived[c], y_send).wait()
        all_of(incoming[c].at[pl.ds(0, (experts - 1) * pairs)], z_send).wait()
    all_of(late_arrived, y_send).wait()
    all_of(late_in.at[pl.ds(1, experts - 1)], z_send).wait()
    all_of(params_arrived, x_send).wait()
    all_of(params_arrived, x_recv).wait()
    flat = params.reshape(blocks, tensors * columns * rows, LANES)
    others = params_arrived.reshape(tensors - 1, blocks, columns * rows, LANES)
    for d in range(1, tensors):
        sender = lax.rem(my_tensor + tensors - d, tensors)
        goal = pl.ds(pl.multiple_of(sender * columns * rows, 8), columns * rows)
        for s in range(blocks):
            flat[s, goal] = others[d - 1, places[s]]


def write_out(*refs):
    half = (len(refs) - 1) // 2
    sems = refs[-1]
    copies = [
        pltpu.make_async_copy(refs[i], refs[half + i], sems.at[i])
        for i in range(half)
    ]
    for copy in copies:
        copy.start()
    for copy in copies:
        copy.wait()


def split(columns):
    middle = columns - LATE - sum(SORTS)
    return [CHUNK] * (middle // CHUNK), list(SORTS), LATE


def body(delta, step_offsets, block_map, master_params, first_moment, second_moment, *, shape):
    replicas, experts, tensors = shape
    blocks, rows_all, width = delta.shape[1:]
    rows = rows_all // replicas
    columns = width // LANES
    pairs = blocks // experts
    chunks, sorts, late = split(columns)
    widths = chunks + sorts
    count = len(widths)
    edge = sum(sorts) + chunks[0]
    terms = delta.reshape(blocks, replicas, rows, columns, LANES).transpose(0, 3, 1, 2, 4)

    def dense(state):
        split = state.reshape(blocks, rows, columns, LANES).transpose(0, 2, 1, 3)
        return split.reshape(blocks, columns * rows, LANES)

    def undense(state):
        split = state.reshape(blocks, columns, rows, LANES).transpose(0, 2, 1, 3)
        return split.reshape(blocks, rows, width)

    state_shape = (blocks, columns * rows, LANES)
    params_shape = (blocks, tensors * columns, rows, LANES)
    anywhere = pl.BlockSpec(memory_space=pltpu.HBM)
    near = pl.BlockSpec(memory_space=pltpu.VMEM)
    dma = pltpu.SemaphoreType.DMA
    sizes = (replicas, experts, tensors, chunks, sorts, late, blocks, pairs, rows)
    piece = (rows, LANES)
    held = pl.pallas_call(
        functools.partial(kernel, sizes),
        out_shape=(
            pltpu.VMEM(params_shape, jnp.bfloat16),
            pltpu.VMEM(state_shape, jnp.float32),
            pltpu.VMEM(state_shape, jnp.float32),
        ),
        in_specs=[anywhere] * 6,
        out_specs=(near,) * 3,
        scratch_shapes=[
            pltpu.VMEM((3,) + state_shape, jnp.float32),
            pltpu.VMEM(state_shape, jnp.float32),
            pltpu.VMEM(state_shape, jnp.float32),
            pltpu.VMEM((blocks, columns) + piece, jnp.bfloat16),
            pltpu.VMEM((blocks, columns) + piece, jnp.bfloat16),
            pltpu.VMEM((tensors - 1, blocks, columns) + piece, jnp.bfloat16),
            pltpu.SMEM(block_map.shape, jnp.int32),
            pltpu.SMEM(step_offsets.shape, jnp.int32),
            pltpu.SMEM((blocks,), jnp.int32),
            pltpu.SMEM((blocks,), jnp.int32),
            pltpu.SMEM((blocks,), jnp.int32),
            dma((2,)),
            dma((2, replicas - 1)),
            dma,
            dma,
            dma,
            dma((count + len(sorts) + 1,)),
            dma,
            dma((count, 3)),
            dma,
            dma,
            dma,
        ]
        + [pltpu.VMEM((replicas - 1, blocks, c) + piece, jnp.bfloat16) for c in (edge, columns - edge)]
        + [pltpu.VMEM((replicas - 1, blocks, c) + piece, jnp.bfloat16) for c in widths]
        + [pltpu.VMEM((blocks, c) + piece, jnp.bfloat16) for c in widths] * 2
        + [pltpu.VMEM((replicas - 1, blocks, c) + piece, jnp.bfloat16) for c in sorts]
        + [pltpu.VMEM((experts, replicas, pairs, late) + piece, jnp.bfloat16)] * 2
        + [pltpu.VMEM((replicas - 1, experts, pairs, late) + piece, jnp.bfloat16)],
        compiler_params=pltpu.CompilerParams(collective_id=0, has_side_effects=True),
    )(block_map, step_offsets, terms, dense(master_params), dense(first_moment), dense(second_moment))
    new_params, new_first, new_second = pl.pallas_call(
        write_out,
        out_shape=(
            jax.ShapeDtypeStruct(params_shape, jnp.bfloat16),
            jax.ShapeDtypeStruct(state_shape, jnp.float32),
            jax.ShapeDtypeStruct(state_shape, jnp.float32),
        ),
        in_specs=[near] * 3,
        out_specs=(anywhere,) * 3,
        scratch_shapes=[dma((3,))],
        compiler_params=pltpu.CompilerParams(vmem_limit_bytes=1024 * 1024),
    )(*held)
    full = new_params.transpose(0, 2, 1, 3).reshape(blocks, rows, tensors * width)
    return (full, undense(new_first), undense(new_second))


def solution(mesh):
    in_specs = (
        P("replica", "expert", None, "tensor"),
        P(),
        P(),
        P("expert", "replica", "tensor"),
        P("expert", "replica", "tensor"),
        P("expert", "replica", "tensor"),
    )
    out_specs = (
        P("expert", "replica", None),
        P("expert", "replica", "tensor"),
        P("expert", "replica", "tensor"),
    )
    shape = tuple(mesh.shape[axis] for axis in ("replica", "expert", "tensor"))
    step = functools.partial(body, shape=shape)
    return jax.shard_map(step, mesh=mesh, in_specs=in_specs, out_specs=out_specs, check_vma=False)
```
